32 devices in a mesh: dp: 8 (over z, y), neg: 4 (over x, core).
Axes of the slice: x: 2, y: 2, z: 4, core: 2. Of those that a mesh axis runs over, the one named last changes fastest.
Arguments:
- query_features: bfloat16 [8192, 512], P(('dp', 'neg')), may hold values from -8 to 8
- positive_features: bfloat16 [8192, 512], P(('dp', 'neg')), may hold values from -6 to 6
- negative_features: bfloat16 [16384, 512], P(('neg', 'dp')), may hold values from -6 to 6
- positive_ids: int32 [8192], P('dp'), may hold values from 0 to 8191, as said below
- positive_counts: int32 [8192], P(('dp', 'neg')), may hold values from 1 to 16
- negative_ids: int32 [16384], P('neg'), may hold values from 0 to 4095, as said below
- negative_counts: int32 [16384], P('neg'), may hold values from 64 to 4096
- query_first: bfloat16 [512, 1024], replicated, may hold values from -0.25 to 0.25
- query_second: bfloat16 [1024, 512], replicated, may hold values from -0.1875 to 0.1875
- query_third: bfloat16 [512, 256], replicated, may hold values from -0.25 to 0.25
- item_first: bfloat16 [512, 1024], replicated, may hold values from -0.25 to 0.25
- item_second: bfloat16 [1024, 512], replicated, may hold values from -0.1875 to 0.1875
- item_third: bfloat16 [512, 256], replicated, may hold values from -0.25 to 0.25
Outputs:
- mean_loss: float32 [], replicated
- clipped_query_first: float32 [512, 1024], P('dp')
- clipped_query_second: float32 [1024, 512], P('dp')
- clipped_query_third: float32 [512, 256], P('dp')
- clipped_item_first: float32 [512, 1024], P('dp')
- clipped_item_second: float32 [1024, 512], P('dp')
- clipped_item_third: float32 [512, 256], P('dp')
The draws below stay inside these ranges and needn't reach their ends.
Inputs may be any that keep to these rules, and one draw needn't show every extreme that they name: `negative_ids`: ids of the sampled negatives; one id may stand for several negatives. `positive_ids`: A query's positive id may equal the ids of some negatives; those negatives are left out of that query's denominator.
All inputs are finite; a program needn't handle non-finite values.
Results may differ from the reference program's by a relative error of at most 0.0075.
Values may be sent and summed in bfloat16 or wider, within the bound.
A program may use at most 128 MiB of HBM per device.

```python
import math
import jax
import jax.numpy as jnp
from jax import lax

FIN = 512
H1 = 1024
H2 = 512
E = 256
NEG = 16384
QUERIES = 8192


def draw_query_features(key, part):
    noise_key, mean_key, scale_key = jax.random.split(key, 3)
    values = jax.random.normal(noise_key, (QUERIES, FIN), jnp.float32)
    return jnp.clip(values, -8.0, 8.0).astype(jnp.bfloat16)


def draw_item_ids(key):
    base = jax.random.fold_in(key, 91)
    pool_key, pick_key, fresh_key, hit_key = jax.random.split(base, 4)
    negatives = jax.random.randint(pool_key, (NEG,), 0, NEG // 4, jnp.int32)
    negatives = negatives.at[0].set(NEG // 4 - 1).at[1].set(0)
    picked = jax.random.randint(pick_key, (QUERIES,), 0, NEG, jnp.int32)
    fresh = jax.random.randint(fresh_key, (QUERIES,), NEG // 4, NEG // 2, jnp.int32)
    choose_hit = jax.random.randint(hit_key, (QUERIES,), 0, 2, jnp.int32)
    positives = jnp.where(choose_hit == 0, negatives[picked], fresh)
    positives = positives.at[0].set(NEG // 2 - 1).at[1].set(0)
    return (negatives, positives)


def draw_negative_ids(key, part):
    return draw_item_ids(key)[0]


def draw_positive_ids(key, part):
    return draw_item_ids(key)[1]


def blocked_counts(key, total, block_rows, low_power, high_power):
    level_key, fine_key = jax.random.split(key)
    levels = jax.random.randint(level_key, (total // block_rows + 1,), low_power, high_power + 1, jnp.int32)
    powers = jnp.left_shift(jnp.ones_like(levels), levels)
    which = jnp.arange(total, dtype=jnp.int32) // block_rows
    base = powers[which]
    fine = jax.random.randint(fine_key, (total,), 0, 65536, jnp.int32) % base
    return base + fine


def draw_negative_counts(key, part):
    counts = blocked_counts(jax.random.fold_in(key, 17), NEG, 256, 6, 11)
    return counts.at[0].set(4096).at[1].set(64)


def draw_positive_counts(key, part):
    counts = blocked_counts(jax.random.fold_in(key, 23), QUERIES, 64, 0, 3)
    return counts.at[0].set(16).at[1].set(1)


def block_scale(key, shape, pieces, least, top_value):
    loudness = 1.0
    for dim, parts in pieces:
        heights = jax.random.uniform(jax.random.fold_in(jax.random.fold_in(key, 6), dim), (parts,), jnp.float32, least / len(pieces), top_value / len(pieces))
        loudness = loudness * jnp.repeat(jnp.exp(heights), shape[dim] // parts).reshape((-1,) + (1,) * (len(shape) - 1 - dim))
    return loudness


def bell_draw(key, shape, scale, limit, shards=(), kind=jnp.bfloat16):
    gain = block_scale(key, shape, shards, -0.22, 0.18) if shards else 1.0
    drawn = jax.random.normal(key, shape, jnp.float32) * scale * gain
    return jnp.minimum(jnp.maximum(drawn, -limit), limit).astype(kind)


def setup_inputs(seed: int = 0) -> dict:
    streams_of = jax.random.split(jax.random.key(seed), 14)
    query_features = draw_query_features(jax.random.fold_in(streams_of[13], 71), 0)
    positive_features = bell_draw(streams_of[1], (QUERIES, FIN), 1.0, 6.0, ((0, 32),))
    negative_features = bell_draw(streams_of[2], (NEG, FIN), 1.0, 6.0, ((0, 32),))
    positive_ids = draw_positive_ids(jax.random.fold_in(streams_of[13], 71), 0)
    positive_counts = draw_positive_counts(jax.random.fold_in(streams_of[13], 71), 0)
    negative_ids = draw_negative_ids(jax.random.fold_in(streams_of[13], 71), 0)
    negative_counts = draw_negative_counts(jax.random.fold_in(streams_of[13], 71), 0)
    query_first = bell_draw(streams_of[7], (FIN, H1), FIN ** -0.5, 0.25)
    query_second = bell_draw(streams_of[8], (H1, H2), H1 ** -0.5, 0.1875)
    query_third = bell_draw(streams_of[9], (H2, E), H2 ** -0.5, 0.25)
    item_first = bell_draw(streams_of[10], (FIN, H1), FIN ** -0.5, 0.25)
    item_second = bell_draw(streams_of[11], (H1, H2), H1 ** -0.5, 0.1875)
    item_third = bell_draw(streams_of[12], (H2, E), H2 ** -0.5, 0.25)
    return dict(query_features=query_features, positive_features=positive_features, negative_features=negative_features, positive_ids=positive_ids, positive_counts=positive_counts, negative_ids=negative_ids, negative_counts=negative_counts, query_first=query_first, query_second=query_second, query_third=query_third, item_first=item_first, item_second=item_second, item_third=item_third)


inv_temp = 20.0
clip_norm = 256.0

def silu_slope(pre):
    sigma = jax.nn.sigmoid(pre)
    return sigma * (1.0 + pre * (1.0 - sigma))

def contract_rows(left, right):
    return lax.dot_general(left, right, (((0,), (0,)), ((), ())), preferred_element_type=jnp.float32)

def contract_cols(left, right):
    return lax.dot_general(left, right, (((1,), (1,)), ((), ())), preferred_element_type=jnp.float32)

def tower_forward(features, first, second, third):
    first_pre = jnp.dot(features, first, preferred_element_type=jnp.float32)
    first_act = jax.nn.silu(first_pre).astype(jnp.bfloat16)
    second_pre = jnp.dot(first_act, second, preferred_element_type=jnp.float32)
    second_act = jax.nn.silu(second_pre).astype(jnp.bfloat16)
    embedding = jnp.dot(second_act, third, preferred_element_type=jnp.float32)
    inv_norm = lax.rsqrt(lax.optimization_barrier(jnp.sum(embedding * embedding, axis=1, keepdims=True)) + 1.0)
    unit = (embedding * inv_norm).astype(jnp.bfloat16)
    return ((first_pre, first_act, second_pre, second_act, embedding, inv_norm), unit)

def tower_backward(features, second, third, saved, unit_grad):
    first_pre, first_act, second_pre, second_act, embedding, inv_norm = saved
    along = lax.optimization_barrier(jnp.sum(embedding * unit_grad, axis=1, keepdims=True))
    embed_grad = (inv_norm * unit_grad - inv_norm * inv_norm * inv_norm * embedding * along).astype(jnp.bfloat16)
    third_grad = contract_rows(second_act, embed_grad)
    second_slope = (contract_cols(embed_grad, third) * silu_slope(second_pre)).astype(jnp.bfloat16)
    second_grad = contract_rows(first_act, second_slope)
    first_slope = (contract_cols(second_slope, second) * silu_slope(first_pre)).astype(jnp.bfloat16)
    first_grad = contract_rows(features, first_slope)
    return (first_grad, second_grad, third_grad)

def reference(query_features, positive_features, negative_features, positive_ids, positive_counts, negative_ids, negative_counts, query_first, query_second, query_third, item_first, item_second, item_third):
    query_saved, query_unit = tower_forward(query_features, query_first, query_second, query_third)
    item_features = jnp.concatenate([positive_features, negative_features], axis=0)
    item_saved, item_unit = tower_forward(item_features, item_first, item_second, item_third)
    positive_unit = item_unit[:QUERIES]
    negative_unit = item_unit[QUERIES:]
    negative_log = jnp.log(negative_counts.astype(jnp.float32))
    positive_logit = lax.optimization_barrier(jnp.sum(query_unit.astype(jnp.float32) * positive_unit.astype(jnp.float32), axis=1)) * inv_temp - jnp.log(positive_counts.astype(jnp.float32))
    block_rows = math.gcd(QUERIES, 2048)
    blocks = QUERIES // block_rows

    def block_step(carry, inputs):
        negative_sum, loss_sum = carry
        query_block, positive_block, logit_block, ids_block = inputs
        scores = contract_cols(query_block, negative_unit) * inv_temp - negative_log[None, :]
        weights = jnp.where(ids_block[:, None] != negative_ids[None, :], jnp.exp(scores), 0.0)
        positive_exp = jnp.exp(logit_block)
        denom = positive_exp + lax.optimization_barrier(jnp.sum(weights, axis=1))
        loss_sum = loss_sum + jnp.sum(jnp.log(denom) - logit_block)
        softmax_weights = (weights / denom[:, None]).astype(jnp.bfloat16)
        positive_slope = positive_exp / denom - 1.0
        query_grad = (jnp.dot(softmax_weights, negative_unit, preferred_element_type=jnp.float32) + positive_slope[:, None] * positive_block.astype(jnp.float32)) * inv_temp
        positive_grad = positive_slope[:, None] * query_block.astype(jnp.float32) * inv_temp
        negative_sum = negative_sum + contract_rows(softmax_weights, query_block)
        return ((negative_sum, loss_sum), (query_grad, positive_grad))
    inputs = (query_unit.reshape(blocks, block_rows, E), positive_unit.reshape(blocks, block_rows, E), positive_logit.reshape(blocks, block_rows), positive_ids.reshape(blocks, block_rows))
    initial = (jnp.zeros((NEG, E), jnp.float32), jnp.zeros((), jnp.float32))
    (negative_sum, loss_sum), (query_grad, positive_grad) = lax.scan(block_step, initial, inputs)
    query_grad = query_grad.reshape(QUERIES, E)
    item_grad = jnp.concatenate([positive_grad.reshape(QUERIES, E), negative_sum * inv_temp], axis=0)
    query_grads = tower_backward(query_features, query_second, query_third, query_saved, query_grad)
    item_grads = tower_backward(item_features, item_second, item_third, item_saved, item_grad)
    gradients = query_grads + item_grads
    squares = jnp.zeros((), jnp.float32)
    for gradient in gradients:
        squares = squares + jnp.sum(gradient * gradient)
    grad_norm = jnp.sqrt(squares)
    clip_factor = clip_norm / jnp.maximum(grad_norm, clip_norm)
    mean_loss = loss_sum / QUERIES
    return (mean_loss, gradients[0] * clip_factor, gradients[1] * clip_factor, gradients[2] * clip_factor, gradients[3] * clip_factor, gradients[4] * clip_factor, gradients[5] * clip_factor)
```

```python
import functools

import jax
import jax.numpy as jnp
from jax import lax
from jax.experimental import pallas as pl
from jax.experimental.pallas import tpu as pltpu
from jax.sharding import PartitionSpec as P

inv_temp = 20.0
clip_norm = 256.0


def silu_slope(pre):
    sigma = jax.nn.sigmoid(pre)
    return sigma * (1.0 + pre * (1.0 - sigma))


def contract_rows(left, right):
    return lax.dot_general(
        left, right, (((0,), (0,)), ((), ())), preferred_element_type=jnp.float32
    )


def contract_cols(left, right):
    return lax.dot_general(
        left, right, (((1,), (1,)), ((), ())), preferred_element_type=jnp.float32
    )


def tower_forward(features, first, second, third):
    first_pre = jnp.dot(features, first, preferred_element_type=jnp.float32)
    first_act = jax.nn.silu(first_pre).astype(jnp.bfloat16)
    second_pre = jnp.dot(first_act, second, preferred_element_type=jnp.float32)
    second_act = jax.nn.silu(second_pre).astype(jnp.bfloat16)
    embedding = jnp.dot(second_act, third, preferred_element_type=jnp.float32)
    inv_norm = lax.rsqrt(jnp.sum(embedding * embedding, axis=1, keepdims=True) + 1.0)
    unit = (embedding * inv_norm).astype(jnp.bfloat16)
    return ((first_pre, first_act, second_pre, second_act, embedding, inv_norm), unit)


def tower_backward(features, second, third, saved, unit_grad):
    first_pre, first_act, second_pre, second_act, embedding, inv_norm = saved
    along = jnp.sum(embedding * unit_grad, axis=1, keepdims=True)
    embed_grad = (inv_norm * unit_grad - inv_norm * inv_norm * inv_norm * embedding * along).astype(
        jnp.bfloat16
    )
    third_grad = contract_rows(second_act, embed_grad)
    second_slope = (contract_cols(embed_grad, third) * silu_slope(second_pre)).astype(jnp.bfloat16)
    second_grad = contract_rows(first_act, second_slope)
    first_slope = (contract_cols(second_slope, second) * silu_slope(first_pre)).astype(jnp.bfloat16)
    first_grad = contract_rows(features, first_slope)
    return (first_grad, second_grad, third_grad)


pack_columns = 256
vmem = pl.BlockSpec(memory_space=pltpu.VMEM)


def greet(ndp, nneg, me_dp, me_neg):
    barrier = pltpu.get_barrier_semaphore()
    for k in range(1, nneg):
        pl.semaphore_signal(
            barrier, inc=1, device_id={"neg": lax.rem(me_neg + k, nneg)}, device_id_type=pl.DeviceIdType.MESH
        )
    for k in range(1, ndp):
        pl.semaphore_signal(
            barrier, inc=1, device_id={"dp": lax.rem(me_dp + k, ndp)}, device_id_type=pl.DeviceIdType.MESH
        )
    pl.semaphore_wait(barrier, (nneg - 1) + (ndp - 1))


def send(src, dst, send_sem, recv_sem, axis, target):
    copy = pltpu.make_async_remote_copy(
        src_ref=src,
        dst_ref=dst,
        send_sem=send_sem,
        recv_sem=recv_sem,
        device_id={axis: target},
        device_id_type=pl.DeviceIdType.MESH,
    )
    copy.start()
    return copy


def share(axis, n, me, src_of, dst, send_sem, recv_sem):
    return [
        send(src_of(lax.rem(me + k, n)), dst.at[me], send_sem.at[k], recv_sem.at[k], axis, lax.rem(me + k, n))
        for k in range(1, n)
    ]


def finish(copies):
    for copy in copies:
        copy.wait()


def gather_kernel(ndp, nneg, query_ref, negative_ref, group_ref, shard_ref, qs, qr, ns, nr):
    me_dp, me_neg = lax.axis_index("dp"), lax.axis_index("neg")
    greet(ndp, nneg, me_dp, me_neg)
    copies = share("dp", ndp, me_dp, lambda t: negative_ref, shard_ref, ns, nr)
    copies += share("neg", nneg, me_neg, lambda t: query_ref, group_ref, qs, qr)
    group_ref[me_neg] = query_ref[...]
    shard_ref[me_dp] = negative_ref[...]
    finish(copies)


def query_kernel(ndp, nneg, part_ref, denom_ref, sum_ref, total_ref, land, denom_land, qs, qr, ds, dr):
    me_dp, me_neg = lax.axis_index("dp"), lax.axis_index("neg")
    greet(1, nneg, me_dp, me_neg)
    small = share("neg", nneg, me_neg, lambda t: denom_ref, denom_land, ds, dr)
    copies = share("neg", nneg, me_neg, lambda t: part_ref.at[t], land, qs, qr)
    total = denom_ref[...]
    finish(small)
    for k in range(1, nneg):
        total = total + denom_land[lax.rem(me_neg + k, nneg)]
    total_ref[...] = total
    finish(copies)
    result = part_ref[me_neg].astype(jnp.float32)
    for k in range(1, nneg):
        result = result + land[lax.rem(me_neg + k, nneg)].astype(jnp.float32)
    sum_ref[...] = result


def negative_kernel(ndp, nneg, part_ref, sum_ref, land, ns, nr):
    me_dp, me_neg = lax.axis_index("dp"), lax.axis_index("neg")
    greet(ndp, 1, me_dp, me_neg)
    copies = share("dp", ndp, me_dp, lambda t: part_ref.at[t], land, ns, nr)
    finish(copies)
    result = part_ref[me_dp].astype(jnp.float32)
    for k in range(1, ndp):
        result = result + land[lax.rem(me_dp + k, ndp)].astype(jnp.float32)
    sum_ref[...] = result


def weight_kernel(
    ndp, nneg, packed_ref, loss_ref, gathered_ref, stats_ref,
    core_land, core_sum, row_land, row_sum, dp_land, stat_dp, stat_dp_land, stat_neg, stat_neg_land,
    cs, cr, xs, xr, ps, pr, ss, sr, ts, tr, gs, gr,
):
    me_dp, me_neg = lax.axis_index("dp"), lax.axis_index("neg")
    nx = nneg // 2
    me_x, me_core = me_neg // 2, lax.rem(me_neg, 2)
    other = 1 - me_core
    greet(ndp, nneg, me_dp, me_neg)
    core = [
        send(packed_ref.at[2 * x + other], core_land.at[x], cs.at[x], cr.at[x], "neg", 2 * me_x + other)
        for x in range(nx)
    ]
    row = []
    for k in list(range(1, nx)) + [0]:
        x = lax.rem(me_x + k, nx)
        if k == 1 or nx == 1:
            finish(core)

        def core_add(d, carry):
            core_sum[x, d] = (
                packed_ref[2 * x + me_core, d].astype(jnp.float32) + core_land[x, d].astype(jnp.float32)
            ).astype(jnp.bfloat16)
            return carry

        lax.fori_loop(0, ndp, core_add, 0)
        if k:
            row.append(
                send(core_sum.at[x], row_land.at[k], xs.at[k], xr.at[k], "neg", 2 * x + me_core)
            )
    finish(row)

    def row_add(d, carry):
        value = core_sum[me_x, d].astype(jnp.float32)
        for k in range(1, nx):
            value = value + row_land[k, d].astype(jnp.float32)
        row_sum[d] = value.astype(jnp.bfloat16)
        return carry

    lax.fori_loop(0, ndp, row_add, 0)
    finish(share("dp", ndp, me_dp, lambda t: row_sum.at[t], dp_land, ps, pr))
    piece = row_sum[me_dp].astype(jnp.float32)
    for k in range(1, ndp):
        piece = piece + dp_land[lax.rem(me_dp + k, ndp)].astype(jnp.float32)
    gathered_ref[me_neg] = piece.astype(jnp.bfloat16)
    lane = lax.broadcasted_iota(jnp.int32, (8, 128), 1)
    stat_dp[...] = jnp.where(lane == 0, jnp.sum(piece * piece), loss_ref[0])
    stat_copies = share("dp", ndp, me_dp, lambda t: stat_dp, stat_dp_land, ss, sr)
    gather = share("neg", nneg, me_neg, lambda t: gathered_ref.at[me_neg], gathered_ref, gs, gr)
    finish(stat_copies)
    total = stat_dp[...]
    for k in range(1, ndp):
        total = total + stat_dp_land[lax.rem(me_dp + k, ndp)]
    stat_neg[...] = total
    finish(share("neg", nneg, me_neg, lambda t: stat_neg, stat_neg_land, ts, tr))
    total = stat_neg[...]
    for k in range(1, nneg):
        total = total + stat_neg_land[lax.rem(me_neg + k, nneg)]
    stats_ref[...] = total
    finish(gather)


def call(kernel, collective, ndp, nneg, out_shape, scratch, in_specs):
    return pl.pallas_call(
        functools.partial(kernel, ndp, nneg),
        out_shape=out_shape,
        in_specs=in_specs,
        out_specs=tuple(vmem for _ in out_shape),
        scratch_shapes=scratch,
        compiler_params=pltpu.CompilerParams(
            collective_id=collective, has_side_effects=True, vmem_limit_bytes=48 * 1024 * 1024
        ),
    )


def sems(*counts):
    return [pltpu.SemaphoreType.DMA((count,)) for count in counts]


def to_packed(gradient, ndp):
    rows, columns = gradient.shape
    blocks = gradient.astype(jnp.bfloat16).reshape(ndp, rows // ndp, columns)
    return [blocks[:, :, c : c + pack_columns] for c in range(0, columns, pack_columns)]


def per_device(
    query_features,
    positive_features,
    negative_features,
    positive_ids,
    positive_counts,
    negative_ids,
    negative_counts,
    query_first,
    query_second,
    query_third,
    item_first,
    item_second,
    item_third,
):
    own_rows = query_features.shape[0]
    query_saved, query_unit = tower_forward(query_features, query_first, query_second, query_third)
    item_features = jnp.concatenate([positive_features, negative_features], axis=0)
    item_saved, item_unit = tower_forward(item_features, item_first, item_second, item_third)
    positive_unit = item_unit[:own_rows]
    negative_unit = item_unit[own_rows:]
    ndp, nneg = lax.axis_size("dp"), lax.axis_size("neg")
    width = query_unit.shape[1]
    group_unit, shard_unit = call(
        gather_kernel,
        0,
        ndp,
        nneg,
        (
            jax.ShapeDtypeStruct((nneg,) + query_unit.shape, jnp.bfloat16),
            jax.ShapeDtypeStruct((ndp,) + negative_unit.shape, jnp.bfloat16),
        ),
        sems(nneg, nneg, ndp, ndp),
        [vmem, vmem],
    )(query_unit, negative_unit)
    group_unit = group_unit.reshape(-1, width)
    shard_unit = shard_unit.reshape(-1, width)
    scores = (
        contract_cols(group_unit, shard_unit) * inv_temp
        - jnp.log(negative_counts.astype(jnp.float32))[None, :]
    )
    weights = jnp.where(positive_ids[:, None] != negative_ids[None, :], jnp.exp(scores), 0.0)
    positive_logit = jnp.sum(
        query_unit.astype(jnp.float32) * positive_unit.astype(jnp.float32), axis=1
    ) * inv_temp - jnp.log(positive_counts.astype(jnp.float32))
    positive_exp = jnp.exp(positive_logit)
    offset = lax.axis_index("neg") * own_rows
    partial_value = jnp.sum(weights, axis=1)
    own_part = lax.dynamic_slice(partial_value, (offset,), (own_rows,)) + positive_exp
    partial_value = lax.dynamic_update_slice(partial_value, own_part, (offset,))
    block = weights.astype(jnp.bfloat16)
    query_part = jnp.dot(block, shard_unit, preferred_element_type=jnp.float32).astype(jnp.bfloat16)
    denom_shape = (nneg * own_rows // 128, 128)
    query_total, denom = call(
        query_kernel,
        1,
        ndp,
        nneg,
        (
            jax.ShapeDtypeStruct((own_rows, width), jnp.float32),
            jax.ShapeDtypeStruct(denom_shape, jnp.float32),
        ),
        [
            pltpu.VMEM((nneg, own_rows, width), jnp.bfloat16),
            pltpu.VMEM((nneg,) + denom_shape, jnp.float32),
        ]
        + sems(nneg, nneg, nneg, nneg),
        [vmem, vmem],
    )(query_part.reshape(nneg, own_rows, width), partial_value.reshape(denom_shape))
    denom = denom.reshape(-1)
    own_denom = lax.dynamic_slice(denom, (offset,), (own_rows,))
    loss_part = jnp.sum(jnp.log(own_denom) - positive_logit)
    positive_slope = positive_exp / own_denom - 1.0
    query_sum = query_total / own_denom[:, None]
    scaled_unit = (group_unit.astype(jnp.float32) / denom[:, None]).astype(jnp.bfloat16)
    negative_part = contract_rows(block, scaled_unit).astype(jnp.bfloat16)
    negative_rows = negative_unit.shape[0]
    (negative_sum,) = call(
        negative_kernel,
        2,
        ndp,
        nneg,
        (jax.ShapeDtypeStruct((negative_rows, width), jnp.float32),),
        [pltpu.VMEM((ndp, negative_rows, width), jnp.bfloat16)] + sems(ndp, ndp),
        [vmem],
    )(negative_part.reshape(ndp, negative_rows, width))
    query_grad = (
        query_sum + positive_slope[:, None] * positive_unit.astype(jnp.float32)
    ) * inv_temp
    positive_grad = positive_slope[:, None] * query_unit.astype(jnp.float32) * inv_temp
    item_grad = jnp.concatenate([positive_grad, negative_sum * inv_temp], axis=0)
    query_grads = tower_backward(query_features, query_second, query_third, query_saved, query_grad)
    item_grads = tower_backward(item_features, item_second, item_third, item_saved, item_grad)
    gradients = query_grads + item_grads
    parts = [part for gradient in gradients for part in to_packed(gradient, ndp)]
    packed = jnp.concatenate(parts, axis=1)
    rows = packed.shape[1] // nneg
    packed = packed.reshape(ndp, nneg, rows, pack_columns).transpose(1, 0, 2, 3)
    nx = nneg // 2
    piece = (rows, pack_columns)
    bf16, f32 = jnp.bfloat16, jnp.float32
    gathered, stats = call(
        weight_kernel,
        3,
        ndp,
        nneg,
        (jax.ShapeDtypeStruct((nneg,) + piece, bf16), jax.ShapeDtypeStruct((8, 128), f32)),
        [
            pltpu.VMEM((nx, ndp) + piece, bf16),
            pltpu.VMEM((nx, ndp) + piece, bf16),
            pltpu.VMEM((nx, ndp) + piece, bf16),
            pltpu.VMEM((ndp,) + piece, bf16),
            pltpu.VMEM((ndp,) + piece, bf16),
            pltpu.VMEM((8, 128), f32),
            pltpu.VMEM((ndp, 8, 128), f32),
            pltpu.VMEM((8, 128), f32),
            pltpu.VMEM((nneg, 8, 128), f32),
        ]
        + sems(nx, nx, nx, nx, ndp, ndp, ndp, ndp, nneg, nneg, nneg, nneg),
        [vmem, pl.BlockSpec(memory_space=pltpu.SMEM)],
    )(packed, loss_part.reshape(1))
    grad_norm = jnp.sqrt(stats[0, 0])
    mean_loss = stats[0, 1] / (own_rows * ndp * nneg)
    clip_factor = clip_norm / jnp.maximum(grad_norm, clip_norm)
    flat = gathered.reshape(nneg * rows, pack_columns)
    clipped = []
    start = 0
    for gradient in gradients:
        height, columns = gradient.shape[0] // ndp, gradient.shape[1]
        groups = columns // pack_columns
        blocks = [flat[start + g * height : start + (g + 1) * height] for g in range(groups)]
        start += groups * height
        clipped.append(jnp.concatenate(blocks, axis=1).astype(jnp.float32) * clip_factor)
    return (mean_loss, *clipped)


def solution(mesh):
    placed = (
        P(("dp", "neg"), None),
        P(("dp", "neg"), None),
        P(("neg", "dp"), None),
        P("dp"),
        P(("dp", "neg")),
        P("neg"),
        P("neg"),
        P(),
        P(),
        P(),
        P(),
        P(),
        P(),
    )
    return jax.shard_map(
        per_device,
        mesh=mesh,
        in_specs=placed,
        out_specs=(
            P(),
            P("dp", None),
            P("dp", None),
            P("dp", None),
            P("dp", None),
            P("dp", None),
            P("dp", None),
        ),
        check_vma=False,
    )
```

```python
import functools

import jax
import jax.numpy as jnp
from jax import lax
from jax.experimental import pallas as pl
from jax.experimental.pallas import tpu as pltpu
from jax.sharding import PartitionSpec as P

inv_temp = 20.0
clip_norm = 256.0


def silu_slope(pre):
    sigma = jax.nn.sigmoid(pre)
    return sigma * (1.0 + pre * (1.0 - sigma))


def contract_rows(left, right):
    return lax.dot_general(
        left, right, (((0,), (0,)), ((), ())), preferred_element_type=jnp.float32
    )


def contract_cols(left, right):
    return lax.dot_general(
        left, right, (((1,), (1,)), ((), ())), preferred_element_type=jnp.float32
    )


def tower_forward(features, first, second, third):
    first_pre = jnp.dot(features, first, preferred_element_type=jnp.float32)
    first_act = jax.nn.silu(first_pre).astype(jnp.bfloat16)
    second_pre = jnp.dot(first_act, second, preferred_element_type=jnp.float32)
    second_act = jax.nn.silu(second_pre).astype(jnp.bfloat16)
    embedding = jnp.dot(second_act, third, preferred_element_type=jnp.float32)
    inv_norm = lax.rsqrt(jnp.sum(embedding * embedding, axis=1, keepdims=True) + 1.0)
    unit = (embedding * inv_norm).astype(jnp.bfloat16)
    return ((first_pre, first_act, second_pre, second_act, embedding, inv_norm), unit)


def tower_backward(features, second, third, saved, unit_grad):
    first_pre, first_act, second_pre, second_act, embedding, inv_norm = saved
    along = jnp.sum(embedding * unit_grad, axis=1, keepdims=True)
    embed_grad = (inv_norm * unit_grad - inv_norm * inv_norm * inv_norm * embedding * along).astype(
        jnp.bfloat16
    )
    third_grad = contract_rows(second_act, embed_grad)
    second_slope = (contract_cols(embed_grad, third) * silu_slope(second_pre)).astype(jnp.bfloat16)
    second_grad = contract_rows(first_act, second_slope)
    first_slope = (contract_cols(second_slope, second) * silu_slope(first_pre)).astype(jnp.bfloat16)
    first_grad = contract_rows(features, first_slope)
    return (first_grad, second_grad, third_grad)


pack_columns = 256
vmem = pl.BlockSpec(memory_space=pltpu.VMEM)


def greet(ndp, nneg, me_dp, me_neg):
    barrier = pltpu.get_barrier_semaphore()
    for k in range(1, nneg):
        pl.semaphore_signal(
            barrier, inc=1, device_id={"neg": lax.rem(me_neg + k, nneg)}, device_id_type=pl.DeviceIdType.MESH
        )
    for k in range(1, ndp):
        pl.semaphore_signal(
            barrier, inc=1, device_id={"dp": lax.rem(me_dp + k, ndp)}, device_id_type=pl.DeviceIdType.MESH
        )
    pl.semaphore_wait(barrier, (nneg - 1) + (ndp - 1))


def send(src, dst, send_sem, recv_sem, axis, target):
    copy = pltpu.make_async_remote_copy(
        src_ref=src,
        dst_ref=dst,
        send_sem=send_sem,
        recv_sem=recv_sem,
        device_id={axis: target},
        device_id_type=pl.DeviceIdType.MESH,
    )
    copy.start()
    return copy


def share(axis, n, me, src_of, dst, send_sem, recv_sem):
    return [
        send(src_of(lax.rem(me + k, n)), dst.at[me], send_sem.at[k], recv_sem.at[k], axis, lax.rem(me + k, n))
        for k in range(1, n)
    ]


def finish(copies):
    for copy in copies:
        copy.wait()


def link(src, dst, sems, index, axis, target):
    send_sems, recv_sems = sems
    return pltpu.make_async_remote_copy(
        src_ref=src,
        dst_ref=dst,
        send_sem=send_sems.at[index],
        recv_sem=recv_sems.at[index],
        device_id={axis: target},
        device_id_type=pl.DeviceIdType.MESH,
    )


def gather_kernel(
    ndp, nneg, query_ref, negative_ref, group_ref, shard_ref, qs, qr, rs, rr, ls, lr, ys, yr
):
    me_dp, me_neg = lax.axis_index("dp"), lax.axis_index("neg")
    line = ndp // 2
    place = me_dp // 2
    partner = me_dp + 1 - 2 * lax.rem(me_dp, 2)
    cuts = negative_ref.shape[0]
    greet(ndp, nneg, me_dp, me_neg)
    goes_right, goes_left = place < line - 1, place > 0

    def block(slot, j, distance):
        return negative_ref.at[j] if distance == 0 else shard_ref.at[slot, j]

    def right(distance, j):
        slot = me_dp - 2 * distance
        return link(block(slot, j, distance), shard_ref.at[slot, j], (rs, rr), (distance + 1) * cuts + j, "dp", lax.rem(me_dp + 2, ndp))

    def left(distance, j):
        slot = me_dp + 2 * distance
        return link(block(slot, j, distance), shard_ref.at[slot, j], (ls, lr), (distance + 1) * cuts + j, "dp", lax.rem(me_dp + ndp - 2, ndp))

    def across(offset, j):
        slot = me_dp + 2 * offset
        return link(block(slot, j, abs(offset)), shard_ref.at[slot, j], (ys, yr), (offset + line - 1) * cuts + j, "dp", partner)

    def arrival(slot, j, sems, index):
        return link(shard_ref.at[slot, j], shard_ref.at[slot, j], sems, index, "dp", partner)

    for j in range(cuts):
        pl.when(goes_right)(lambda j=j: right(0, j).start())
        pl.when(goes_left)(lambda j=j: left(0, j).start())
        across(0, j).start()
    copies = share("neg", nneg, me_neg, lambda t: query_ref, group_ref, qs, qr)
    group_ref[me_neg] = query_ref[...]
    shard_ref[me_dp] = negative_ref[...]
    for distance in range(1, line):
        for j in range(cuts):

            @pl.when(place >= distance)
            def _():
                arrival(me_dp - 2 * distance, j, (rs, rr), distance * cuts + j).wait_recv()
                across(-distance, j).start()
                pl.when(goes_right)(lambda: right(distance, j).start())

            @pl.when(place + distance < line)
            def _():
                arrival(me_dp + 2 * distance, j, (ls, lr), distance * cuts + j).wait_recv()
                across(distance, j).start()
                pl.when(goes_left)(lambda: left(distance, j).start())

    for distance in range(line):
        for j in range(cuts):

            @pl.when(place >= distance)
            def _():
                across(-distance, j).wait_send()
                arrival(partner - 2 * distance, j, (ys, yr), (line - 1 - distance) * cuts + j).wait_recv()
                pl.when(goes_right)(lambda: right(distance, j).wait_send())

            @pl.when(place + distance < line)
            def _():
                if distance:
                    across(distance, j).wait_send()
                    arrival(partner + 2 * distance, j, (ys, yr), (line - 1 + distance) * cuts + j).wait_recv()
                pl.when(goes_left)(lambda: left(distance, j).wait_send())

    finish(copies)


def query_kernel(ndp, nneg, part_ref, denom_ref, sum_ref, total_ref, land, denom_land, qs, qr, ds, dr):
    me_dp, me_neg = lax.axis_index("dp"), lax.axis_index("neg")
    greet(1, nneg, me_dp, me_neg)
    small = share("neg", nneg, me_neg, lambda t: denom_ref, denom_land, ds, dr)
    copies = share("neg", nneg, me_neg, lambda t: part_ref.at[t], land, qs, qr)
    total = denom_ref[...]
    finish(small)
    for k in range(1, nneg):
        total = total + denom_land[lax.rem(me_neg + k, nneg)]
    total_ref[...] = total
    finish(copies)
    result = part_ref[me_neg].astype(jnp.float32)
    for k in range(1, nneg):
        result = result + land[lax.rem(me_neg + k, nneg)].astype(jnp.float32)
    sum_ref[...] = result


def negative_kernel(
    ndp, nneg, part_ref, sum_ref, pair_land, right_land, left_land, right_sum, left_sum, ys, yr, rs, rr, ls, lr
):
    me_dp, me_neg = lax.axis_index("dp"), lax.axis_index("neg")
    line = ndp // 2
    place, side = me_dp // 2, lax.rem(me_dp, 2)
    partner = me_dp + 1 - 2 * side
    cuts = part_ref.shape[1]
    greet(ndp, 1, me_dp, me_neg)
    order = sorted(range(line), key=lambda z: -abs(2 * z - line + 1))
    steps = [(z, j) for z in order for j in range(cuts)]
    from_left, from_right = place > 0, place < line - 1

    def across(z, j):
        return link(part_ref.at[2 * z + 1 - side, j], pair_land.at[z, j], (ys, yr), z * cuts + j, "dp", partner)

    def right(z, j):
        return link(right_sum.at[z, j], right_land.at[z, j], (rs, rr), z * cuts + j, "dp", lax.rem(me_dp + 2, ndp))

    def left(z, j):
        return link(left_sum.at[z, j], left_land.at[z, j], (ls, lr), z * cuts + j, "dp", lax.rem(me_dp + ndp - 2, ndp))

    for z, j in steps:
        across(z, j).start()
    for z, j in steps:
        across(z, j).wait_recv()
        own = part_ref[2 * z + side, j].astype(jnp.float32) + pair_land[z, j].astype(jnp.float32)

        @pl.when(place == z)
        def _():
            sum_ref[j] = own

        @pl.when(place == 0 if z else False)
        def _():
            right_sum[z, j] = own.astype(jnp.bfloat16)

        @pl.when((place > 0) & (place < z))
        def _():
            right(z, j).wait_recv()
            right_sum[z, j] = (own + right_land[z, j].astype(jnp.float32)).astype(jnp.bfloat16)

        pl.when(place < z)(lambda: right(z, j).start())

        @pl.when(place == line - 1 if z < line - 1 else False)
        def _():
            left_sum[z, j] = own.astype(jnp.bfloat16)

        @pl.when((place < line - 1) & (place > z))
        def _():
            left(z, j).wait_recv()
            left_sum[z, j] = (own + left_land[z, j].astype(jnp.float32)).astype(jnp.bfloat16)

        pl.when(place > z)(lambda: left(z, j).start())

    for j in range(cuts):

        @pl.when(from_left)
        def _():
            right(place, j).wait_recv()
            sum_ref[j] = sum_ref[j] + right_land[place, j].astype(jnp.float32)

        @pl.when(from_right)
        def _():
            left(place, j).wait_recv()
            sum_ref[j] = sum_ref[j] + left_land[place, j].astype(jnp.float32)

    for z, j in steps:
        across(z, j).wait_send()
        pl.when(place < z)(lambda: right(z, j).wait_send())
        pl.when(place > z)(lambda: left(z, j).wait_send())


def weight_kernel(
    ndp, nneg, packed_ref, loss_ref, gathered_ref, stats_ref,
    core_land, sum_a, sum_b, land_a, land_b, half_a, half_b, last_a, last_b, line_sum, line_land,
    stat_dp, stat_dp_land, stat_neg, stat_neg_land,
    cs, cr, xs, xr, ys, yr, ps, pr, ss, sr, ts, tr, gs, gr, hs, hr,
):
    me_dp, me_neg = lax.axis_index("dp"), lax.axis_index("neg")
    nx, line = nneg // 2, ndp // 2
    me_x, me_core = me_neg // 2, lax.rem(me_neg, 2)
    place, side = me_dp // 2, lax.rem(me_dp, 2)
    other, far = 1 - me_core, 1 - side
    mate, partner = 2 * me_x + other, 2 * place + far
    greet(ndp, nneg, me_dp, me_neg)
    turn = list(range(1, nx)) + [0]

    def x_of(k):
        return lax.rem(me_x + k, nx)

    core = {}
    for k in turn:
        x = x_of(k)
        core[k] = send(packed_ref.at[2 * x + other], core_land.at[x], cs.at[k], cr.at[k], "neg", mate)

    def add_core(x, y, half, target):
        def body(z, carry):
            target[z] = (
                packed_ref[2 * x + me_core, 2 * z + y, half].astype(jnp.float32)
                + core_land[x, 2 * z + y, half].astype(jnp.float32)
            ).astype(jnp.bfloat16)
            return carry

        lax.fori_loop(0, line, body, 0)

    def add(target, *terms):
        def body(z, carry):
            value = terms[0][z].astype(jnp.float32)
            for term in terms[1:]:
                value = value + term[z].astype(jnp.float32)
            target[z] = value.astype(jnp.bfloat16)
            return carry

        lax.fori_loop(0, line, body, 0)

    first_a = []
    for k in turn:
        x = x_of(k)
        core[k].wait_recv()
        if k:
            for y in range(2):
                add_core(x, y, 0, sum_a.at[x, y])
            first_a.append(send(sum_a.at[x], land_a.at[k], xs.at[k], xr.at[k], "neg", 2 * x + me_core))
        add_core(x, far, 1, sum_b.at[far, x])
    first_b = send(sum_b.at[far], land_b, ys.at[0], yr.at[0], "dp", partner)
    for y in range(2):
        add_core(me_x, y, 0, sum_a.at[me_x, y])
    for k in range(nx):
        add_core(x_of(k), side, 1, sum_b.at[side, x_of(k)])
    for copy in first_a:
        copy.wait_recv()
    add(half_a.at[far], sum_a.at[me_x, far], *[land_a.at[k, far] for k in range(1, nx)])
    second_a = send(half_a.at[far], last_a, ys.at[1], yr.at[1], "dp", partner)
    first_b.wait_recv()
    second_b = []
    for k in turn:
        x = x_of(k)
        add(half_b.at[x], sum_b.at[side, x], land_b.at[x])
        if k:
            second_b.append(
                send(half_b.at[x], last_b.at[k], xs.at[nx + k], xr.at[nx + k], "neg", 2 * x + me_core)
            )
    add(half_a.at[side], sum_a.at[me_x, side], *[land_a.at[k, side] for k in range(1, nx)])
    second_a.wait_recv()
    add(line_sum.at[0], half_a.at[side], last_a)
    third = []
    for half in range(2):
        if half:
            for copy in second_b:
                copy.wait_recv()
            add(line_sum.at[1], half_b.at[me_x], *[last_b.at[k] for k in range(1, nx)])
        for k in range(1, line):
            z = lax.rem(place + k, line)
            third.append(
                send(line_sum.at[half, z], line_land.at[half, k], ps.at[half * line + k], pr.at[half * line + k], "dp", 2 * z + side)
            )
    for copy in third:
        copy.wait_recv()
    squares = jnp.zeros((), jnp.float32)
    for half in range(2):
        piece = line_sum[half, place].astype(jnp.float32)
        for k in range(1, line):
            piece = piece + line_land[half, k].astype(jnp.float32)
        gathered_ref[me_neg, half] = piece.astype(jnp.bfloat16)
        squares = squares + jnp.sum(piece * piece)
    lane = lax.broadcasted_iota(jnp.int32, (8, 128), 1)
    stat_dp[...] = jnp.where(lane == 0, squares, loss_ref[0])
    stat_copies = share("dp", ndp, me_dp, lambda t: stat_dp, stat_dp_land, ss, sr)
    mine = gathered_ref.at[me_neg]
    spread = [send(mine, mine, gs.at[k], gr.at[k], "neg", 2 * x_of(k) + me_core) for k in range(1, nx)]
    spread.append(send(mine, mine, gs.at[0], gr.at[0], "neg", mate))
    finish(stat_copies)
    total = stat_dp[...]
    for k in range(1, ndp):
        total = total + stat_dp_land[lax.rem(me_dp + k, ndp)]
    stat_neg[...] = total
    stat_copies = share("neg", nneg, me_neg, lambda t: stat_neg, stat_neg_land, ts, tr)
    relay = []
    for k in range(1, nx):
        spread[k - 1].wait_recv()
        x = lax.rem(me_x + nx - k, nx)
        came = gathered_ref.at[2 * x + me_core]
        relay.append(send(came, came, hs.at[k], hr.at[k], "neg", mate))
    finish(stat_copies)
    total = stat_neg[...]
    for k in range(1, nneg):
        total = total + stat_neg_land[lax.rem(me_neg + k, nneg)]
    stats_ref[...] = total
    spread[-1].wait_recv()
    finish(relay)
    for copy in [*core.values(), *first_a, first_b, second_a, *second_b, *third, *spread]:
        copy.wait_send()


def call(kernel, collective, ndp, nneg, out_shape, scratch, in_specs):
    return pl.pallas_call(
        functools.partial(kernel, ndp, nneg),
        out_shape=out_shape,
        in_specs=in_specs,
        out_specs=tuple(vmem for _ in out_shape),
        scratch_shapes=scratch,
        compiler_params=pltpu.CompilerParams(
            collective_id=collective, has_side_effects=True, vmem_limit_bytes=48 * 1024 * 1024
        ),
    )


def sems(*counts):
    return [pltpu.SemaphoreType.DMA((count,)) for count in counts]


def to_packed(gradient, ndp):
    rows, columns = gradient.shape
    blocks = gradient.astype(jnp.bfloat16).reshape(ndp, rows // ndp, columns)
    return [blocks[:, :, c : c + pack_columns] for c in range(0, columns, pack_columns)]


def per_device(
    query_features,
    positive_features,
    negative_features,
    positive_ids,
    positive_counts,
    negative_ids,
    negative_counts,
    query_first,
    query_second,
    query_third,
    item_first,
    item_second,
    item_third,
):
    own_rows = query_features.shape[0]
    query_saved, query_unit = tower_forward(query_features, query_first, query_second, query_third)
    item_features = jnp.concatenate([positive_features, negative_features], axis=0)
    item_saved, item_unit = tower_forward(item_features, item_first, item_second, item_third)
    positive_unit = item_unit[:own_rows]
    negative_unit = item_unit[own_rows:]
    ndp, nneg = lax.axis_size("dp"), lax.axis_size("neg")
    width = query_unit.shape[1]
    cuts = 2
    cut_rows = negative_unit.shape[0] // cuts
    group_unit, shard_unit = call(
        gather_kernel,
        0,
        ndp,
        nneg,
        (
            jax.ShapeDtypeStruct((nneg,) + query_unit.shape, jnp.bfloat16),
            jax.ShapeDtypeStruct((ndp, cuts, cut_rows, width), jnp.bfloat16),
        ),
        sems(nneg, nneg, *([ndp // 2 * cuts + cuts] * 4), *([ndp * cuts] * 2)),
        [vmem, vmem],
    )(query_unit, negative_unit.reshape(cuts, cut_rows, width))
    group_unit = group_unit.reshape(-1, width)
    shard_unit = shard_unit.reshape(-1, width)
    scores = (
        contract_cols(group_unit, shard_unit) * inv_temp
        - jnp.log(negative_counts.astype(jnp.float32))[None, :]
    )
    weights = jnp.where(positive_ids[:, None] != negative_ids[None, :], jnp.exp(scores), 0.0)
    positive_logit = jnp.sum(
        query_unit.astype(jnp.float32) * positive_unit.astype(jnp.float32), axis=1
    ) * inv_temp - jnp.log(positive_counts.astype(jnp.float32))
    positive_exp = jnp.exp(positive_logit)
    offset = lax.axis_index("neg") * own_rows
    partial_value = jnp.sum(weights, axis=1)
    own_part = lax.dynamic_slice(partial_value, (offset,), (own_rows,)) + positive_exp
    partial_value = lax.dynamic_update_slice(partial_value, own_part, (offset,))
    block = weights.astype(jnp.bfloat16)
    query_part = jnp.dot(block, shard_unit, preferred_element_type=jnp.float32).astype(jnp.bfloat16)
    denom_shape = (nneg * own_rows // 128, 128)
    query_total, denom = call(
        query_kernel,
        1,
        ndp,
        nneg,
        (
            jax.ShapeDtypeStruct((own_rows, width), jnp.float32),
            jax.ShapeDtypeStruct(denom_shape, jnp.float32),
        ),
        [
            pltpu.VMEM((nneg, own_rows, width), jnp.bfloat16),
            pltpu.VMEM((nneg,) + denom_shape, jnp.float32),
        ]
        + sems(nneg, nneg, nneg, nneg),
        [vmem, vmem],
    )(query_part.reshape(nneg, own_rows, width), partial_value.reshape(denom_shape))
    denom = denom.reshape(-1)
    own_denom = lax.dynamic_slice(denom, (offset,), (own_rows,))
    loss_part = jnp.sum(jnp.log(own_denom) - positive_logit)
    positive_slope = positive_exp / own_denom - 1.0
    query_sum = query_total / own_denom[:, None]
    scaled_unit = (group_unit.astype(jnp.float32) / denom[:, None]).astype(jnp.bfloat16)
    negative_part = contract_rows(block, scaled_unit).astype(jnp.bfloat16)
    line = ndp // 2
    cut = (cuts, cut_rows, width)
    (negative_sum,) = call(
        negative_kernel,
        2,
        ndp,
        nneg,
        (jax.ShapeDtypeStruct(cut, jnp.float32),),
        [pltpu.VMEM((line,) + cut, jnp.bfloat16)] * 5 + sems(*([line * cuts] * 6)),
        [vmem],
    )(negative_part.reshape((ndp,) + cut))
    negative_sum = negative_sum.reshape(negative_unit.shape)
    query_grad = (
        query_sum + positive_slope[:, None] * positive_unit.astype(jnp.float32)
    ) * inv_temp
    positive_grad = positive_slope[:, None] * query_unit.astype(jnp.float32) * inv_temp
    item_grad = jnp.concatenate([positive_grad, negative_sum * inv_temp], axis=0)
    query_grads = tower_backward(query_features, query_second, query_third, query_saved, query_grad)
    item_grads = tower_backward(item_features, item_second, item_third, item_saved, item_grad)
    gradients = query_grads + item_grads
    parts = [part for gradient in gradients for part in to_packed(gradient, ndp)]
    packed = jnp.concatenate(parts, axis=1)
    rows = packed.shape[1] // nneg
    packed = packed.reshape(ndp, nneg, 2, rows // 2, pack_columns).transpose(1, 0, 2, 3, 4)
    nx = nneg // 2
    piece = (rows // 2, pack_columns)
    bf16, f32 = jnp.bfloat16, jnp.float32
    gathered, stats = call(
        weight_kernel,
        3,
        ndp,
        nneg,
        (jax.ShapeDtypeStruct((nneg, 2) + piece, bf16), jax.ShapeDtypeStruct((8, 128), f32)),
        [
            pltpu.VMEM((nx, ndp, 2) + piece, bf16),
            pltpu.VMEM((nx, 2, line) + piece, bf16),
            pltpu.VMEM((2, nx, line) + piece, bf16),
            pltpu.VMEM((nx, 2, line) + piece, bf16),
            pltpu.VMEM((nx, line) + piece, bf16),
            pltpu.VMEM((2, line) + piece, bf16),
            pltpu.VMEM((nx, line) + piece, bf16),
            pltpu.VMEM((line,) + piece, bf16),
            pltpu.VMEM((nx, line) + piece, bf16),
            pltpu.VMEM((2, line) + piece, bf16),
            pltpu.VMEM((2, line) + piece, bf16),
            pltpu.VMEM((8, 128), f32),
            pltpu.VMEM((ndp, 8, 128), f32),
            pltpu.VMEM((8, 128), f32),
            pltpu.VMEM((nneg, 8, 128), f32),
        ]
        + sems(nx, nx, 2 * nx, 2 * nx, 2, 2, ndp, ndp, ndp, ndp, nneg, nneg, nx, nx, nx, nx),
        [vmem, pl.BlockSpec(memory_space=pltpu.SMEM)],
    )(packed, loss_part.reshape(1))
    grad_norm = jnp.sqrt(stats[0, 0])
    mean_loss = stats[0, 1] / (own_rows * ndp * nneg)
    clip_factor = clip_norm / jnp.maximum(grad_norm, clip_norm)
    flat = gathered.reshape(nneg * rows, pack_columns)
    clipped = []
    start = 0
    for gradient in gradients:
        height, columns = gradient.shape[0] // ndp, gradient.shape[1]
        groups = columns // pack_columns
        blocks = [flat[start + g * height : start + (g + 1) * height] for g in range(groups)]
        start += groups * height
        clipped.append(jnp.concatenate(blocks, axis=1).astype(jnp.float32) * clip_factor)
    return (mean_loss, *clipped)


def solution(mesh):
    placed = (
        P(("dp", "neg"), None),
        P(("dp", "neg"), None),
        P(("neg", "dp"), None),
        P("dp"),
        P(("dp", "neg")),
        P("neg"),
        P("neg"),
        P(),
        P(),
        P(),
        P(),
        P(),
        P(),
    )
    return jax.shard_map(
        per_device,
        mesh=mesh,
        in_specs=placed,
        out_specs=(
            P(),
            P("dp", None),
            P("dp", None),
            P("dp", None),
            P("dp", None),
            P("dp", None),
            P("dp", None),
        ),
        check_vma=False,
    )
```

```python
import functools

import jax
import jax.numpy as jnp
from jax import lax
from jax.experimental import pallas as pl
from jax.experimental.pallas import tpu as pltpu
from jax.sharding import PartitionSpec as P

inv_temp = 20.0
clip_norm = 256.0


def silu_slope(pre):
    sigma = jax.nn.sigmoid(pre)
    return sigma * (1.0 + pre * (1.0 - sigma))


def contract_rows(left, right):
    return lax.dot_general(
        left, right, (((0,), (0,)), ((), ())), preferred_element_type=jnp.float32
    )


def contract_cols(left, right):
    return lax.dot_general(
        left, right, (((1,), (1,)), ((), ())), preferred_element_type=jnp.float32
    )


def tower_forward(features, first, second, third):
    first_pre = jnp.dot(features, first, preferred_element_type=jnp.float32)
    first_act = jax.nn.silu(first_pre).astype(jnp.bfloat16)
    second_pre = jnp.dot(first_act, second, preferred_element_type=jnp.float32)
    second_act = jax.nn.silu(second_pre).astype(jnp.bfloat16)
    embedding = jnp.dot(second_act, third, preferred_element_type=jnp.float32)
    inv_norm = lax.rsqrt(jnp.sum(embedding * embedding, axis=1, keepdims=True) + 1.0)
    unit = (embedding * inv_norm).astype(jnp.bfloat16)
    return ((first_pre, first_act, second_pre, second_act, embedding, inv_norm), unit)


def tower_backward(features, second, third, saved, unit_grad):
    first_pre, first_act, second_pre, second_act, embedding, inv_norm = saved
    along = jnp.sum(embedding * unit_grad, axis=1, keepdims=True)
    embed_grad = (inv_norm * unit_grad - inv_norm * inv_norm * inv_norm * embedding * along).astype(
        jnp.bfloat16
    )
    third_grad = contract_rows(second_act, embed_grad)
    second_slope = (contract_cols(embed_grad, third) * silu_slope(second_pre)).astype(jnp.bfloat16)
    second_grad = contract_rows(first_act, second_slope)
    first_slope = (contract_cols(second_slope, second) * silu_slope(first_pre)).astype(jnp.bfloat16)
    first_grad = contract_rows(features, first_slope)
    return (first_grad, second_grad, third_grad)


pack_columns = 256
vmem = pl.BlockSpec(memory_space=pltpu.VMEM)


def greet(ndp, nneg, me_dp, me_neg):
    barrier = pltpu.get_barrier_semaphore()
    for k in range(1, nneg):
        pl.semaphore_signal(
            barrier, inc=1, device_id={"neg": lax.rem(me_neg + k, nneg)}, device_id_type=pl.DeviceIdType.MESH
        )
    for k in range(1, ndp):
        pl.semaphore_signal(
            barrier, inc=1, device_id={"dp": lax.rem(me_dp + k, ndp)}, device_id_type=pl.DeviceIdType.MESH
        )
    pl.semaphore_wait(barrier, (nneg - 1) + (ndp - 1))


def send(src, dst, send_sem, recv_sem, axis, target):
    copy = pltpu.make_async_remote_copy(
        src_ref=src,
        dst_ref=dst,
        send_sem=send_sem,
        recv_sem=recv_sem,
        device_id={axis: target},
        device_id_type=pl.DeviceIdType.MESH,
    )
    copy.start()
    return copy


def share(axis, n, me, src_of, dst, send_sem, recv_sem):
    return [
        send(src_of(lax.rem(me + k, n)), dst.at[me], send_sem.at[k], recv_sem.at[k], axis, lax.rem(me + k, n))
        for k in range(1, n)
    ]


def finish(copies):
    for copy in copies:
        copy.wait()


def link(src, dst, sems, index, axis, target):
    send_sems, recv_sems = sems
    return pltpu.make_async_remote_copy(
        src_ref=src,
        dst_ref=dst,
        send_sem=send_sems.at[index],
        recv_sem=recv_sems.at[index],
        device_id={axis: target},
        device_id_type=pl.DeviceIdType.MESH,
    )


def gather_kernel(
    ndp, nneg, query_ref, negative_ref, group_ref, shard_ref, qs, qr, rs, rr, ls, lr, ys, yr
):
    me_dp, me_neg = lax.axis_index("dp"), lax.axis_index("neg")
    line = ndp // 2
    place = me_dp // 2
    partner = me_dp + 1 - 2 * lax.rem(me_dp, 2)
    greet(ndp, nneg, me_dp, me_neg)
    goes_right, goes_left = place < line - 1, place > 0

    def at(lane, offset):
        slot = (partner if lane == 2 else me_dp) + 2 * offset
        return shard_ref.at[slot, min(lane, 1)]

    def source(lane, offset):
        return negative_ref.at[lane] if offset == 0 and lane < 2 else at(lane, offset)

    def right(lane, distance):
        return link(source(lane, -distance), at(lane, -distance), (rs, rr), (distance + 1) * 3 + lane, "dp", lax.rem(me_dp + 2, ndp))

    def left(lane, distance):
        return link(source(lane, distance), at(lane, distance), (ls, lr), (distance + 1) * 3 + lane, "dp", lax.rem(me_dp + ndp - 2, ndp))

    def across(offset):
        return link(source(0, offset), at(0, offset), (ys, yr), offset + line - 1, "dp", partner)

    def across_second():
        return link(negative_ref.at[1], at(1, 0), (ys, yr), 2 * line - 1, "dp", partner)

    def arrival(ref, sems, index):
        return link(ref, ref, sems, index, "dp", partner)

    def begin(lane):
        pl.when(goes_right)(lambda: right(lane, 0).start())
        pl.when(goes_left)(lambda: left(lane, 0).start())

    across_second().start()
    begin(0)
    begin(1)
    across(0).start()
    copies = share("neg", nneg, me_neg, lambda t: query_ref, group_ref, qs, qr)
    group_ref[me_neg] = query_ref[...]
    shard_ref[me_dp] = negative_ref[...]
    arrival(at(2, 0), (ys, yr), 2 * line - 1).wait_recv()
    begin(2)
    for distance in range(1, line):
        for lane in range(3):

            @pl.when(place >= distance)
            def _():
                arrival(at(lane, -distance), (rs, rr), distance * 3 + lane).wait_recv()
                if lane == 0:
                    across(-distance).start()
                pl.when(goes_right)(lambda: right(lane, distance).start())

            @pl.when(place + distance < line)
            def _():
                arrival(at(lane, distance), (ls, lr), distance * 3 + lane).wait_recv()
                if lane == 0:
                    across(distance).start()
                pl.when(goes_left)(lambda: left(lane, distance).start())

    across_second().wait_send()
    for distance in range(line):

        @pl.when(place >= distance)
        def _():
            across(-distance).wait_send()
            arrival(shard_ref.at[partner - 2 * distance, 0], (ys, yr), line - 1 - distance).wait_recv()
            for lane in range(3):
                pl.when(goes_right)(lambda: right(lane, distance).wait_send())

        @pl.when(place + distance < line)
        def _():
            if distance:
                across(distance).wait_send()
                arrival(shard_ref.at[partner + 2 * distance, 0], (ys, yr), line - 1 + distance).wait_recv()
            for lane in range(3):
                pl.when(goes_left)(lambda: left(lane, distance).wait_send())

    finish(copies)


def query_kernel(ndp, nneg, part_ref, denom_ref, sum_ref, total_ref, land, denom_land, qs, qr, ds, dr):
    me_dp, me_neg = lax.axis_index("dp"), lax.axis_index("neg")
    greet(1, nneg, me_dp, me_neg)
    small = share("neg", nneg, me_neg, lambda t: denom_ref, denom_land, ds, dr)
    copies = share("neg", nneg, me_neg, lambda t: part_ref.at[t], land, qs, qr)
    total = denom_ref[...]
    finish(small)
    for k in range(1, nneg):
        total = total + denom_land[lax.rem(me_neg + k, nneg)]
    total_ref[...] = total
    finish(copies)
    result = part_ref[me_neg].astype(jnp.float32)
    for k in range(1, nneg):
        result = result + land[lax.rem(me_neg + k, nneg)].astype(jnp.float32)
    sum_ref[...] = result


def negative_kernel(
    ndp, nneg, part_ref, sum_ref, pair_land, right_land, left_land, right_sum, left_sum, far_sum, far_send, far_land,
    ys, yr, rs, rr, ls, lr,
):
    me_dp, me_neg = lax.axis_index("dp"), lax.axis_index("neg")
    line = ndp // 2
    place, side = me_dp // 2, lax.rem(me_dp, 2)
    partner = me_dp + 1 - 2 * side
    greet(ndp, 1, me_dp, me_neg)
    order = sorted(range(line), key=lambda z: -abs(2 * z - line + 1))
    from_left, from_right = place > 0, place < line - 1

    def across(z):
        return link(part_ref.at[2 * z + 1 - side, 0], pair_land.at[z], (ys, yr), z, "dp", partner)

    def right(z, lane):
        return link(right_sum.at[z, lane], right_land.at[z, lane], (rs, rr), z * 3 + lane, "dp", lax.rem(me_dp + 2, ndp))

    def left(z, lane):
        return link(left_sum.at[z, lane], left_land.at[z, lane], (ls, lr), z * 3 + lane, "dp", lax.rem(me_dp + ndp - 2, ndp))

    def total(lane):
        return far_sum if lane == 2 else sum_ref.at[lane]

    for z in order:
        across(z).start()
    for z in order:
        for lane in (1, 2, 0):
            if lane == 0:
                across(z).wait_recv()
                own = part_ref[2 * z + side, 0].astype(jnp.float32) + pair_land[z].astype(jnp.float32)
            else:
                own = part_ref[2 * z + (side if lane == 1 else 1 - side), 1].astype(jnp.float32)

            @pl.when(place == z)
            def _():
                total(lane)[...] = own

            @pl.when(place == 0 if z else False)
            def _():
                right_sum[z, lane] = own.astype(jnp.bfloat16)

            @pl.when((place > 0) & (place < z))
            def _():
                right(z, lane).wait_recv()
                right_sum[z, lane] = (own + right_land[z, lane].astype(jnp.float32)).astype(jnp.bfloat16)

            pl.when(place < z)(lambda: right(z, lane).start())

            @pl.when(place == line - 1 if z < line - 1 else False)
            def _():
                left_sum[z, lane] = own.astype(jnp.bfloat16)

            @pl.when((place < line - 1) & (place > z))
            def _():
                left(z, lane).wait_recv()
                left_sum[z, lane] = (own + left_land[z, lane].astype(jnp.float32)).astype(jnp.bfloat16)

            pl.when(place > z)(lambda: left(z, lane).start())

    second = link(far_send, far_land, (ys, yr), line, "dp", partner)
    for lane in (2, 1, 0):

        @pl.when(from_left)
        def _():
            right(place, lane).wait_recv()
            total(lane)[...] = total(lane)[...] + right_land[place, lane].astype(jnp.float32)

        @pl.when(from_right)
        def _():
            left(place, lane).wait_recv()
            total(lane)[...] = total(lane)[...] + left_land[place, lane].astype(jnp.float32)

        if lane == 2:
            far_send[...] = far_sum[...].astype(jnp.bfloat16)
            second.start()

    second.wait()
    sum_ref[1] = sum_ref[1] + far_land[...].astype(jnp.float32)
    for z in order:
        across(z).wait_send()
        for lane in range(3):
            pl.when(place < z)(lambda: right(z, lane).wait_send())
            pl.when(place > z)(lambda: left(z, lane).wait_send())


def weight_kernel(
    ndp, nneg, packed_ref, loss_ref, gathered_ref, stats_ref,
    core_land, sum_a, sum_b, land_a, land_b, half_a, half_b, last_a, last_b, line_sum, line_land,
    stat_dp, stat_dp_land, stat_neg, stat_neg_land,
    cs, cr, xs, xr, ys, yr, ps, pr, ss, sr, ts, tr, gs, gr, hs, hr,
):
    me_dp, me_neg = lax.axis_index("dp"), lax.axis_index("neg")
    nx, line = nneg // 2, ndp // 2
    me_x, me_core = me_neg // 2, lax.rem(me_neg, 2)
    place, side = me_dp // 2, lax.rem(me_dp, 2)
    other, far = 1 - me_core, 1 - side
    mate, partner = 2 * me_x + other, 2 * place + far
    greet(ndp, nneg, me_dp, me_neg)
    turn = list(range(1, nx)) + [0]

    def x_of(k):
        return lax.rem(me_x + k, nx)

    core = {}
    for k in turn:
        x = x_of(k)
        core[k] = send(packed_ref.at[2 * x + other], core_land.at[x], cs.at[k], cr.at[k], "neg", mate)

    def add_core(x, y, half, target):
        def body(z, carry):
            target[z] = (
                packed_ref[2 * x + me_core, 2 * z + y, half].astype(jnp.float32)
                + core_land[x, 2 * z + y, half].astype(jnp.float32)
            ).astype(jnp.bfloat16)
            return carry

        lax.fori_loop(0, line, body, 0)

    def add(target, *terms):
        def body(z, carry):
            value = terms[0][z].astype(jnp.float32)
            for term in terms[1:]:
                value = value + term[z].astype(jnp.float32)
            target[z] = value.astype(jnp.bfloat16)
            return carry

        lax.fori_loop(0, line, body, 0)

    first_a = []
    for k in turn:
        x = x_of(k)
        core[k].wait_recv()
        if k:
            for y in range(2):
                add_core(x, y, 0, sum_a.at[x, y])
            first_a.append(send(sum_a.at[x], land_a.at[k], xs.at[k], xr.at[k], "neg", 2 * x + me_core))
        add_core(x, far, 1, sum_b.at[far, x])
    first_b = send(sum_b.at[far], land_b, ys.at[0], yr.at[0], "dp", partner)
    for y in range(2):
        add_core(me_x, y, 0, sum_a.at[me_x, y])
    for k in range(nx):
        add_core(x_of(k), side, 1, sum_b.at[side, x_of(k)])
    for copy in first_a:
        copy.wait_recv()
    add(half_a.at[far], sum_a.at[me_x, far], *[land_a.at[k, far] for k in range(1, nx)])
    second_a = send(half_a.at[far], last_a, ys.at[1], yr.at[1], "dp", partner)
    first_b.wait_recv()
    second_b = []
    for k in turn:
        x = x_of(k)
        add(half_b.at[x], sum_b.at[side, x], land_b.at[x])
        if k:
            second_b.append(
                send(half_b.at[x], last_b.at[k], xs.at[nx + k], xr.at[nx + k], "neg", 2 * x + me_core)
            )
    add(half_a.at[side], sum_a.at[me_x, side], *[land_a.at[k, side] for k in range(1, nx)])
    second_a.wait_recv()
    add(line_sum.at[0], half_a.at[side], last_a)
    third = []
    for half in range(2):
        if half:
            for copy in second_b:
                copy.wait_recv()
            add(line_sum.at[1], half_b.at[me_x], *[last_b.at[k] for k in range(1, nx)])
        for k in range(1, line):
            z = lax.rem(place + k, line)
            third.append(
                send(line_sum.at[half, z], line_land.at[half, k], ps.at[half * line + k], pr.at[half * line + k], "dp", 2 * z + side)
            )
    for copy in third:
        copy.wait_recv()
    squares = jnp.zeros((), jnp.float32)
    for half in range(2):
        piece = line_sum[half, place].astype(jnp.float32)
        for k in range(1, line):
            piece = piece + line_land[half, k].astype(jnp.float32)
        gathered_ref[me_neg, half] = piece.astype(jnp.bfloat16)
        squares = squares + jnp.sum(piece * piece)
    lane = lax.broadcasted_iota(jnp.int32, (8, 128), 1)
    stat_dp[...] = jnp.where(lane == 0, squares, loss_ref[0])
    stat_copies = share("dp", ndp, me_dp, lambda t: stat_dp, stat_dp_land, ss, sr)
    mine = gathered_ref.at[me_neg]
    spread = [send(mine, mine, gs.at[k], gr.at[k], "neg", 2 * x_of(k) + me_core) for k in range(1, nx)]
    spread.append(send(mine, mine, gs.at[0], gr.at[0], "neg", mate))
    finish(stat_copies)
    total = stat_dp[...]
    for k in range(1, ndp):
        total = total + stat_dp_land[lax.rem(me_dp + k, ndp)]
    stat_neg[...] = total
    stat_copies = share("neg", nneg, me_neg, lambda t: stat_neg, stat_neg_land, ts, tr)
    relay = []
    for k in range(1, nx):
        spread[k - 1].wait_recv()
        x = lax.rem(me_x + nx - k, nx)
        came = gathered_ref.at[2 * x + me_core]
        relay.append(send(came, came, hs.at[k], hr.at[k], "neg", mate))
    finish(stat_copies)
    total = stat_neg[...]
    for k in range(1, nneg):
        total = total + stat_neg_land[lax.rem(me_neg + k, nneg)]
    stats_ref[...] = total
    spread[-1].wait_recv()
    finish(relay)
    for copy in [*core.values(), *first_a, first_b, second_a, *second_b, *third, *spread]:
        copy.wait_send()


def call(kernel, collective, ndp, nneg, out_shape, scratch, in_specs):
    return pl.pallas_call(
        functools.partial(kernel, ndp, nneg),
        out_shape=out_shape,
        in_specs=in_specs,
        out_specs=tuple(vmem for _ in out_shape),
        scratch_shapes=scratch,
        compiler_params=pltpu.CompilerParams(
            collective_id=collective, has_side_effects=True, vmem_limit_bytes=48 * 1024 * 1024
        ),
    )


def sems(*counts):
    return [pltpu.SemaphoreType.DMA((count,)) for count in counts]


def to_packed(gradient, ndp):
    rows, columns = gradient.shape
    blocks = gradient.astype(jnp.bfloat16).reshape(ndp, rows // ndp, columns)
    return [blocks[:, :, c : c + pack_columns] for c in range(0, columns, pack_columns)]


def per_device(
    query_features,
    positive_features,
    negative_features,
    positive_ids,
    positive_counts,
    negative_ids,
    negative_counts,
    query_first,
    query_second,
    query_third,
    item_first,
    item_second,
    item_third,
):
    own_rows = query_features.shape[0]
    query_saved, query_unit = tower_forward(query_features, query_first, query_second, query_third)
    item_features = jnp.concatenate([positive_features, negative_features], axis=0)
    item_saved, item_unit = tower_forward(item_features, item_first, item_second, item_third)
    positive_unit = item_unit[:own_rows]
    negative_unit = item_unit[own_rows:]
    ndp, nneg = lax.axis_size("dp"), lax.axis_size("neg")
    width = query_unit.shape[1]
    cuts = 2
    cut_rows = negative_unit.shape[0] // cuts
    group_unit, shard_unit = call(
        gather_kernel,
        0,
        ndp,
        nneg,
        (
            jax.ShapeDtypeStruct((nneg,) + query_unit.shape, jnp.bfloat16),
            jax.ShapeDtypeStruct((ndp, cuts, cut_rows, width), jnp.bfloat16),
        ),
        sems(nneg, nneg, *([ndp // 2 * 3 + 3] * 4), ndp, ndp),
        [vmem, vmem],
    )(query_unit, negative_unit.reshape(cuts, cut_rows, width))
    group_unit = group_unit.reshape(-1, width)
    shard_unit = shard_unit.reshape(-1, width)
    scores = (
        contract_cols(group_unit, shard_unit) * inv_temp
        - jnp.log(negative_counts.astype(jnp.float32))[None, :]
    )
    weights = jnp.where(positive_ids[:, None] != negative_ids[None, :], jnp.exp(scores), 0.0)
    positive_logit = jnp.sum(
        query_unit.astype(jnp.float32) * positive_unit.astype(jnp.float32), axis=1
    ) * inv_temp - jnp.log(positive_counts.astype(jnp.float32))
    positive_exp = jnp.exp(positive_logit)
    offset = lax.axis_index("neg") * own_rows
    partial_value = jnp.sum(weights, axis=1)
    own_part = lax.dynamic_slice(partial_value, (offset,), (own_rows,)) + positive_exp
    partial_value = lax.dynamic_update_slice(partial_value, own_part, (offset,))
    block = weights.astype(jnp.bfloat16)
    query_part = jnp.dot(block, shard_unit, preferred_element_type=jnp.float32).astype(jnp.bfloat16)
    denom_shape = (nneg * own_rows // 128, 128)
    query_total, denom = call(
        query_kernel,
        1,
        ndp,
        nneg,
        (
            jax.ShapeDtypeStruct((own_rows, width), jnp.float32),
            jax.ShapeDtypeStruct(denom_shape, jnp.float32),
        ),
        [
            pltpu.VMEM((nneg, own_rows, width), jnp.bfloat16),
            pltpu.VMEM((nneg,) + denom_shape, jnp.float32),
        ]
        + sems(nneg, nneg, nneg, nneg),
        [vmem, vmem],
    )(query_part.reshape(nneg, own_rows, width), partial_value.reshape(denom_shape))
    denom = denom.reshape(-1)
    own_denom = lax.dynamic_slice(denom, (offset,), (own_rows,))
    loss_part = jnp.sum(jnp.log(own_denom) - positive_logit)
    positive_slope = positive_exp / own_denom - 1.0
    query_sum = query_total / own_denom[:, None]
    scaled_unit = (group_unit.astype(jnp.float32) / denom[:, None]).astype(jnp.bfloat16)
    negative_part = contract_rows(block, scaled_unit).astype(jnp.bfloat16)
    line = ndp // 2
    cut = (cuts, cut_rows, width)
    (negative_sum,) = call(
        negative_kernel,
        2,
        ndp,
        nneg,
        (jax.ShapeDtypeStruct(cut, jnp.float32),),
        [pltpu.VMEM((line,) + cut[1:], jnp.bfloat16)]
        + [pltpu.VMEM((line, 3) + cut[1:], jnp.bfloat16)] * 4
        + [pltpu.VMEM(cut[1:], kind) for kind in (jnp.float32, jnp.bfloat16, jnp.bfloat16)]
        + sems(line + 1, line + 1, *([line * 3] * 4)),
        [vmem],
    )(negative_part.reshape((ndp,) + cut))
    negative_sum = negative_sum.reshape(negative_unit.shape)
    query_grad = (
        query_sum + positive_slope[:, None] * positive_unit.astype(jnp.float32)
    ) * inv_temp
    positive_grad = positive_slope[:, None] * query_unit.astype(jnp.float32) * inv_temp
    item_grad = jnp.concatenate([positive_grad, negative_sum * inv_temp], axis=0)
    query_grads = tower_backward(query_features, query_second, query_third, query_saved, query_grad)
    item_grads = tower_backward(item_features, item_second, item_third, item_saved, item_grad)
    gradients = query_grads + item_grads
    parts = [part for gradient in gradients for part in to_packed(gradient, ndp)]
    packed = jnp.concatenate(parts, axis=1)
    rows = packed.shape[1] // nneg
    packed = packed.reshape(ndp, nneg, 2, rows // 2, pack_columns).transpose(1, 0, 2, 3, 4)
    nx = nneg // 2
    piece = (rows // 2, pack_columns)
    bf16, f32 = jnp.bfloat16, jnp.float32
    gathered, stats = call(
        weight_kernel,
        3,
        ndp,
        nneg,
        (jax.ShapeDtypeStruct((nneg, 2) + piece, bf16), jax.ShapeDtypeStruct((8, 128), f32)),
        [
            pltpu.VMEM((nx, ndp, 2) + piece, bf16),
            pltpu.VMEM((nx, 2, line) + piece, bf16),
            pltpu.VMEM((2, nx, line) + piece, bf16),
            pltpu.VMEM((nx, 2, line) + piece, bf16),
            pltpu.VMEM((nx, line) + piece, bf16),
            pltpu.VMEM((2, line) + piece, bf16),
            pltpu.VMEM((nx, line) + piece, bf16),
            pltpu.VMEM((line,) + piece, bf16),
            pltpu.VMEM((nx, line) + piece, bf16),
            pltpu.VMEM((2, line) + piece, bf16),
            pltpu.VMEM((2, line) + piece, bf16),
            pltpu.VMEM((8, 128), f32),
            pltpu.VMEM((ndp, 8, 128), f32),
            pltpu.VMEM((8, 128), f32),
            pltpu.VMEM((nneg, 8, 128), f32),
        ]
        + sems(nx, nx, 2 * nx, 2 * nx, 2, 2, ndp, ndp, ndp, ndp, nneg, nneg, nx, nx, nx, nx),
        [vmem, pl.BlockSpec(memory_space=pltpu.SMEM)],
    )(packed, loss_part.reshape(1))
    grad_norm = jnp.sqrt(stats[0, 0])
    mean_loss = stats[0, 1] / (own_rows * ndp * nneg)
    clip_factor = clip_norm / jnp.maximum(grad_norm, clip_norm)
    flat = gathered.reshape(nneg * rows, pack_columns)
    clipped = []
    start = 0
    for gradient in gradients:
        height, columns = gradient.shape[0] // ndp, gradient.shape[1]
        groups = columns // pack_columns
        blocks = [flat[start + g * height : start + (g + 1) * height] for g in range(groups)]
        start += groups * height
        clipped.append(jnp.concatenate(blocks, axis=1).astype(jnp.float32) * clip_factor)
    return (mean_loss, *clipped)


def solution(mesh):
    placed = (
        P(("dp", "neg"), None),
        P(("dp", "neg"), None),
        P(("neg", "dp"), None),
        P("dp"),
        P(("dp", "neg")),
        P("neg"),
        P("neg"),
        P(),
        P(),
        P(),
        P(),
        P(),
        P(),
    )
    return jax.shard_map(
        per_device,
        mesh=mesh,
        in_specs=placed,
        out_specs=(
            P(),
            P("dp", None),
            P("dp", None),
            P("dp", None),
            P("dp", None),
            P("dp", None),
            P("dp", None),
        ),
        check_vma=False,
    )
```

```python
import functools

import jax
import jax.numpy as jnp
from jax import lax
from jax.experimental import pallas as pl
from jax.experimental.pallas import tpu as pltpu
from jax.sharding import PartitionSpec as P

inv_temp = 20.0
clip_norm = 256.0


def silu_slope(pre):
    sigma = jax.nn.sigmoid(pre)
    return sigma * (1.0 + pre * (1.0 - sigma))


def contract_rows(left, right):
    return lax.dot_general(
        left, right, (((0,), (0,)), ((), ())), preferred_element_type=jnp.float32
    )


def contract_cols(left, right):
    return lax.dot_general(
        left, right, (((1,), (1,)), ((), ())), preferred_element_type=jnp.float32
    )


def tower_forward(features, first, second, third):
    first_pre = jnp.dot(features, first, preferred_element_type=jnp.float32)
    first_act = jax.nn.silu(first_pre).astype(jnp.bfloat16)
    second_pre = jnp.dot(first_act, second, preferred_element_type=jnp.float32)
    second_act = jax.nn.silu(second_pre).astype(jnp.bfloat16)
    embedding = jnp.dot(second_act, third, preferred_element_type=jnp.float32)
    inv_norm = lax.rsqrt(jnp.sum(embedding * embedding, axis=1, keepdims=True) + 1.0)
    unit = (embedding * inv_norm).astype(jnp.bfloat16)
    return ((first_pre, first_act, second_pre, second_act, embedding, inv_norm), unit)


def tower_backward(features, second, third, saved, unit_grad):
    first_pre, first_act, second_pre, second_act, embedding, inv_norm = saved
    along = jnp.sum(embedding * unit_grad, axis=1, keepdims=True)
    embed_grad = (inv_norm * unit_grad - inv_norm * inv_norm * inv_norm * embedding * along).astype(
        jnp.bfloat16
    )
    third_grad = contract_rows(second_act, embed_grad)
    second_slope = (contract_cols(embed_grad, third) * silu_slope(second_pre)).astype(jnp.bfloat16)
    second_grad = contract_rows(first_act, second_slope)
    first_slope = (contract_cols(second_slope, second) * silu_slope(first_pre)).astype(jnp.bfloat16)
    first_grad = contract_rows(features, first_slope)
    return (first_grad, second_grad, third_grad)


pack_columns = 256
vmem = pl.BlockSpec(memory_space=pltpu.VMEM)


def greet(ndp, nneg, me_dp, me_neg):
    barrier = pltpu.get_barrier_semaphore()
    for k in range(1, nneg):
        pl.semaphore_signal(
            barrier, inc=1, device_id={"neg": lax.rem(me_neg + k, nneg)}, device_id_type=pl.DeviceIdType.MESH
        )
    for k in range(1, ndp):
        pl.semaphore_signal(
            barrier, inc=1, device_id={"dp": lax.rem(me_dp + k, ndp)}, device_id_type=pl.DeviceIdType.MESH
        )
    pl.semaphore_wait(barrier, (nneg - 1) + (ndp - 1))


def send(src, dst, send_sem, recv_sem, axis, target):
    copy = pltpu.make_async_remote_copy(
        src_ref=src,
        dst_ref=dst,
        send_sem=send_sem,
        recv_sem=recv_sem,
        device_id={axis: target},
        device_id_type=pl.DeviceIdType.MESH,
    )
    copy.start()
    return copy


def share(axis, n, me, src_of, dst, send_sem, recv_sem):
    return [
        send(src_of(lax.rem(me + k, n)), dst.at[me], send_sem.at[k], recv_sem.at[k], axis, lax.rem(me + k, n))
        for k in range(1, n)
    ]


def finish(copies):
    for copy in copies:
        copy.wait()


def link(src, dst, sems, index, axis, target):
    send_sems, recv_sems = sems
    return pltpu.make_async_remote_copy(
        src_ref=src,
        dst_ref=dst,
        send_sem=send_sems.at[index],
        recv_sem=recv_sems.at[index],
        device_id={axis: target},
        device_id_type=pl.DeviceIdType.MESH,
    )


def gather_kernel(
    ndp, nneg, query_ref, negative_ref, group_ref, shard_ref, qs, qr, rs, rr, ls, lr, ys, yr
):
    me_dp, me_neg = lax.axis_index("dp"), lax.axis_index("neg")
    line = ndp // 2
    place = me_dp // 2
    partner = me_dp + 1 - 2 * lax.rem(me_dp, 2)
    cuts = negative_ref.shape[0]
    greet(ndp, nneg, me_dp, me_neg)
    goes_right, goes_left = place < line - 1, place > 0

    def block(slot, j, distance):
        return negative_ref.at[j] if distance == 0 else shard_ref.at[slot, j]

    def right(distance, j):
        slot = me_dp - 2 * distance
        return link(block(slot, j, distance), shard_ref.at[slot, j], (rs, rr), (distance + 1) * cuts + j, "dp", lax.rem(me_dp + 2, ndp))

    def left(distance, j):
        slot = me_dp + 2 * distance
        return link(block(slot, j, distance), shard_ref.at[slot, j], (ls, lr), (distance + 1) * cuts + j, "dp", lax.rem(me_dp + ndp - 2, ndp))

    def across(offset, j):
        slot = me_dp + 2 * offset
        return link(block(slot, j, abs(offset)), shard_ref.at[slot, j], (ys, yr), (offset + line - 1) * cuts + j, "dp", partner)

    def arrival(slot, j, sems, index):
        return link(shard_ref.at[slot, j], shard_ref.at[slot, j], sems, index, "dp", partner)

    for j in range(cuts):
        pl.when(goes_right)(lambda j=j: right(0, j).start())
        pl.when(goes_left)(lambda j=j: left(0, j).start())
        across(0, j).start()
    copies = share("neg", nneg, me_neg, lambda t: query_ref, group_ref, qs, qr)
    group_ref[me_neg] = query_ref[...]
    shard_ref[me_dp] = negative_ref[...]
    for distance in range(1, line):
        for j in range(cuts):

            @pl.when(place >= distance)
            def _():
                arrival(me_dp - 2 * distance, j, (rs, rr), distance * cuts + j).wait_recv()
                across(-distance, j).start()
                pl.when(goes_right)(lambda: right(distance, j).start())

            @pl.when(place + distance < line)
            def _():
                arrival(me_dp + 2 * distance, j, (ls, lr), distance * cuts + j).wait_recv()
                across(distance, j).start()
                pl.when(goes_left)(lambda: left(distance, j).start())

    for distance in range(line):
        for j in range(cuts):

            @pl.when(place >= distance)
            def _():
                across(-distance, j).wait_send()
                arrival(partner - 2 * distance, j, (ys, yr), (line - 1 - distance) * cuts + j).wait_recv()
                pl.when(goes_right)(lambda: right(distance, j).wait_send())

            @pl.when(place + distance < line)
            def _():
                if distance:
                    across(distance, j).wait_send()
                    arrival(partner + 2 * distance, j, (ys, yr), (line - 1 + distance) * cuts + j).wait_recv()
                pl.when(goes_left)(lambda: left(distance, j).wait_send())

    finish(copies)


def query_kernel(ndp, nneg, part_ref, denom_ref, sum_ref, total_ref, land, denom_land, qs, qr, ds, dr):
    me_dp, me_neg = lax.axis_index("dp"), lax.axis_index("neg")
    greet(1, nneg, me_dp, me_neg)
    small = share("neg", nneg, me_neg, lambda t: denom_ref, denom_land, ds, dr)
    copies = share("neg", nneg, me_neg, lambda t: part_ref.at[t], land, qs, qr)
    total = denom_ref[...]
    finish(small)
    for k in range(1, nneg):
        total = total + denom_land[lax.rem(me_neg + k, nneg)]
    total_ref[...] = total
    finish(copies)
    result = part_ref[me_neg].astype(jnp.float32)
    for k in range(1, nneg):
        result = result + land[lax.rem(me_neg + k, nneg)].astype(jnp.float32)
    sum_ref[...] = result


def negative_kernel(
    ndp, nneg, part_ref, sum_ref, pair_land, right_land, left_land, right_sum, left_sum, ys, yr, rs, rr, ls, lr
):
    me_dp, me_neg = lax.axis_index("dp"), lax.axis_index("neg")
    line = ndp // 2
    place, side = me_dp // 2, lax.rem(me_dp, 2)
    partner = me_dp + 1 - 2 * side
    cuts = part_ref.shape[1]
    greet(ndp, 1, me_dp, me_neg)
    order = sorted(range(line), key=lambda z: -abs(2 * z - line + 1))
    steps = [(z, j) for z in order for j in range(cuts)]
    from_left, from_right = place > 0, place < line - 1

    def across(z, j):
        return link(part_ref.at[2 * z + 1 - side, j], pair_land.at[z, j], (ys, yr), z * cuts + j, "dp", partner)

    def right(z, j):
        return link(right_sum.at[z, j], right_land.at[z, j], (rs, rr), z * cuts + j, "dp", lax.rem(me_dp + 2, ndp))

    def left(z, j):
        return link(left_sum.at[z, j], left_land.at[z, j], (ls, lr), z * cuts + j, "dp", lax.rem(me_dp + ndp - 2, ndp))

    for z, j in steps:
        across(z, j).start()
    for z, j in steps:
        across(z, j).wait_recv()
        own = part_ref[2 * z + side, j].astype(jnp.float32) + pair_land[z, j].astype(jnp.float32)

        @pl.when(place == z)
        def _():
            sum_ref[j] = own

        @pl.when(place == 0 if z else False)
        def _():
            right_sum[z, j] = own.astype(jnp.bfloat16)

        @pl.when((place > 0) & (place < z))
        def _():
            right(z, j).wait_recv()
            right_sum[z, j] = (own + right_land[z, j].astype(jnp.float32)).astype(jnp.bfloat16)

        pl.when(place < z)(lambda: right(z, j).start())

        @pl.when(place == line - 1 if z < line - 1 else False)
        def _():
            left_sum[z, j] = own.astype(jnp.bfloat16)

        @pl.when((place < line - 1) & (place > z))
        def _():
            left(z, j).wait_recv()
            left_sum[z, j] = (own + left_land[z, j].astype(jnp.float32)).astype(jnp.bfloat16)

        pl.when(place > z)(lambda: left(z, j).start())

    for j in range(cuts):

        @pl.when(from_left)
        def _():
            right(place, j).wait_recv()
            sum_ref[j] = sum_ref[j] + right_land[place, j].astype(jnp.float32)

        @pl.when(from_right)
        def _():
            left(place, j).wait_recv()
            sum_ref[j] = sum_ref[j] + left_land[place, j].astype(jnp.float32)

    for z, j in steps:
        across(z, j).wait_send()
        pl.when(place < z)(lambda: right(z, j).wait_send())
        pl.when(place > z)(lambda: left(z, j).wait_send())


def weight_kernel(
    ndp, nneg, packed_ref, loss_ref, gathered_ref, stats_ref,
    core_land, sum_a, sum_b, land_a, land_b, half_a, half_b, last_a, last_b, line_sum, line_land,
    stat_dp, stat_dp_land, stat_neg, stat_neg_land,
    cs, cr, xs, xr, ys, yr, ps, pr, ss, sr, ts, tr, gs, gr, hs, hr,
):
    me_dp, me_neg = lax.axis_index("dp"), lax.axis_index("neg")
    nx, line = nneg // 2, ndp // 2
    me_x, me_core = me_neg // 2, lax.rem(me_neg, 2)
    place, side = me_dp // 2, lax.rem(me_dp, 2)
    other, far = 1 - me_core, 1 - side
    mate, partner = 2 * me_x + other, 2 * place + far
    greet(ndp, nneg, me_dp, me_neg)
    turn = list(range(1, nx)) + [0]

    def x_of(k):
        return lax.rem(me_x + k, nx)

    core = {}
    for k in turn:
        x = x_of(k)
        core[k] = send(packed_ref.at[2 * x + other], core_land.at[x], cs.at[k], cr.at[k], "neg", mate)

    def add_core(x, y, half, target):
        def body(z, carry):
            target[z] = (
                packed_ref[2 * x + me_core, 2 * z + y, half].astype(jnp.float32)
                + core_land[x, 2 * z + y, half].astype(jnp.float32)
            ).astype(jnp.bfloat16)
            return carry

        lax.fori_loop(0, line, body, 0)

    def add(target, *terms):
        def body(z, carry):
            value = terms[0][z].astype(jnp.float32)
            for term in terms[1:]:
                value = value + term[z].astype(jnp.float32)
            target[z] = value.astype(jnp.bfloat16)
            return carry

        lax.fori_loop(0, line, body, 0)

    first_a = []
    for k in turn:
        x = x_of(k)
        core[k].wait_recv()
        if k:
            for y in range(2):
                add_core(x, y, 0, sum_a.at[x, y])
            first_a.append(send(sum_a.at[x], land_a.at[k], xs.at[k], xr.at[k], "neg", 2 * x + me_core))
        add_core(x, far, 1, sum_b.at[far, x])
    first_b = send(sum_b.at[far], land_b, ys.at[0], yr.at[0], "dp", partner)
    for y in range(2):
        add_core(me_x, y, 0, sum_a.at[me_x, y])
    for k in range(nx):
        add_core(x_of(k), side, 1, sum_b.at[side, x_of(k)])
    for copy in first_a:
        copy.wait_recv()
    add(half_a.at[far], sum_a.at[me_x, far], *[land_a.at[k, far] for k in range(1, nx)])
    second_a = send(half_a.at[far], last_a, ys.at[1], yr.at[1], "dp", partner)
    first_b.wait_recv()
    second_b = []
    for k in turn:
        x = x_of(k)
        add(half_b.at[x], sum_b.at[side, x], land_b.at[x])
        if k:
            second_b.append(
                send(half_b.at[x], last_b.at[k], xs.at[nx + k], xr.at[nx + k], "neg", 2 * x + me_core)
            )
    add(half_a.at[side], sum_a.at[me_x, side], *[land_a.at[k, side] for k in range(1, nx)])
    second_a.wait_recv()
    add(line_sum.at[0], half_a.at[side], last_a)
    third = []
    for half in range(2):
        if half:
            for copy in second_b:
                copy.wait_recv()
            add(line_sum.at[1], half_b.at[me_x], *[last_b.at[k] for k in range(1, nx)])
        for k in range(1, line):
            z = lax.rem(place + k, line)
            third.append(
                send(line_sum.at[half, z], line_land.at[half, k], ps.at[half * line + k], pr.at[half * line + k], "dp", 2 * z + side)
            )
    for copy in third:
        copy.wait_recv()
    squares = jnp.zeros((), jnp.float32)
    for half in range(2):
        piece = line_sum[half, place].astype(jnp.float32)
        for k in range(1, line):
            piece = piece + line_land[half, k].astype(jnp.float32)
        gathered_ref[me_neg, half] = piece.astype(jnp.bfloat16)
        squares = squares + jnp.sum(piece * piece)
    lane = lax.broadcasted_iota(jnp.int32, (8, 128), 1)
    stat_dp[...] = jnp.where(lane == 0, squares, loss_ref[0])
    stat_copies = share("dp", ndp, me_dp, lambda t: stat_dp, stat_dp_land, ss, sr)
    mine = gathered_ref.at[me_neg]
    spread = [send(mine, mine, gs.at[k], gr.at[k], "neg", 2 * x_of(k) + me_core) for k in range(1, nx)]
    spread.append(send(mine, mine, gs.at[0], gr.at[0], "neg", mate))
    finish(stat_copies)
    total = stat_dp[...]
    for k in range(1, ndp):
        total = total + stat_dp_land[lax.rem(me_dp + k, ndp)]
    stat_neg[...] = total
    stat_copies = share("neg", nneg, me_neg, lambda t: stat_neg, stat_neg_land, ts, tr)
    relay = []
    for k in range(1, nx):
        spread[k - 1].wait_recv()
        x = lax.rem(me_x + nx - k, nx)
        came = gathered_ref.at[2 * x + me_core]
        relay.append(send(came, came, hs.at[k], hr.at[k], "neg", mate))
    finish(stat_copies)
    total = stat_neg[...]
    for k in range(1, nneg):
        total = total + stat_neg_land[lax.rem(me_neg + k, nneg)]
    stats_ref[...] = total
    spread[-1].wait_recv()
    finish(relay)
    for copy in [*core.values(), *first_a, first_b, second_a, *second_b, *third, *spread]:
        copy.wait_send()


def call(kernel, collective, ndp, nneg, out_shape, scratch, in_specs):
    return pl.pallas_call(
        functools.partial(kernel, ndp, nneg),
        out_shape=out_shape,
        in_specs=in_specs,
        out_specs=tuple(vmem for _ in out_shape),
        scratch_shapes=scratch,
        compiler_params=pltpu.CompilerParams(
            collective_id=collective, has_side_effects=True, vmem_limit_bytes=48 * 1024 * 1024
        ),
    )


def sems(*counts):
    return [pltpu.SemaphoreType.DMA((count,)) for count in counts]


def to_packed(gradient, ndp):
    rows, columns = gradient.shape
    blocks = gradient.astype(jnp.bfloat16).reshape(ndp, rows // ndp, columns)
    return [blocks[:, :, c : c + pack_columns] for c in range(0, columns, pack_columns)]


def per_device(
    query_features,
    positive_features,
    negative_features,
    positive_ids,
    positive_counts,
    negative_ids,
    negative_counts,
    query_first,
    query_second,
    query_third,
    item_first,
    item_second,
    item_third,
):
    own_rows = query_features.shape[0]
    query_saved, query_unit = tower_forward(query_features, query_first, query_second, query_third)
    item_features = jnp.concatenate([positive_features, negative_features], axis=0)
    item_saved, item_unit = tower_forward(item_features, item_first, item_second, item_third)
    positive_unit = item_unit[:own_rows]
    negative_unit = item_unit[own_rows:]
    ndp, nneg = lax.axis_size("dp"), lax.axis_size("neg")
    width = query_unit.shape[1]
    cuts = 4
    cut_rows = negative_unit.shape[0] // cuts
    group_unit, shard_unit = call(
        gather_kernel,
        0,
        ndp,
        nneg,
        (
            jax.ShapeDtypeStruct((nneg,) + query_unit.shape, jnp.bfloat16),
            jax.ShapeDtypeStruct((ndp, cuts, cut_rows, width), jnp.bfloat16),
        ),
        sems(nneg, nneg, *([ndp // 2 * cuts + cuts] * 4), *([ndp * cuts] * 2)),
        [vmem, vmem],
    )(query_unit, negative_unit.reshape(cuts, cut_rows, width))
    group_unit = group_unit.reshape(-1, width)
    shard_unit = shard_unit.reshape(-1, width)
    scores = (
        contract_cols(group_unit, shard_unit) * inv_temp
        - jnp.log(negative_counts.astype(jnp.float32))[None, :]
    )
    weights = jnp.where(positive_ids[:, None] != negative_ids[None, :], jnp.exp(scores), 0.0)
    positive_logit = jnp.sum(
        query_unit.astype(jnp.float32) * positive_unit.astype(jnp.float32), axis=1
    ) * inv_temp - jnp.log(positive_counts.astype(jnp.float32))
    positive_exp = jnp.exp(positive_logit)
    offset = lax.axis_index("neg") * own_rows
    partial_value = jnp.sum(weights, axis=1)
    own_part = lax.dynamic_slice(partial_value, (offset,), (own_rows,)) + positive_exp
    partial_value = lax.dynamic_update_slice(partial_value, own_part, (offset,))
    block = weights.astype(jnp.bfloat16)
    query_part = jnp.dot(block, shard_unit, preferred_element_type=jnp.float32).astype(jnp.bfloat16)
    denom_shape = (nneg * own_rows // 128, 128)
    query_total, denom = call(
        query_kernel,
        1,
        ndp,
        nneg,
        (
            jax.ShapeDtypeStruct((own_rows, width), jnp.float32),
            jax.ShapeDtypeStruct(denom_shape, jnp.float32),
        ),
        [
            pltpu.VMEM((nneg, own_rows, width), jnp.bfloat16),
            pltpu.VMEM((nneg,) + denom_shape, jnp.float32),
        ]
        + sems(nneg, nneg, nneg, nneg),
        [vmem, vmem],
    )(query_part.reshape(nneg, own_rows, width), partial_value.reshape(denom_shape))
    denom = denom.reshape(-1)
    own_denom = lax.dynamic_slice(denom, (offset,), (own_rows,))
    loss_part = jnp.sum(jnp.log(own_denom) - positive_logit)
    positive_slope = positive_exp / own_denom - 1.0
    query_sum = query_total / own_denom[:, None]
    scaled_unit = (group_unit.astype(jnp.float32) / denom[:, None]).astype(jnp.bfloat16)
    negative_part = contract_rows(block, scaled_unit).astype(jnp.bfloat16)
    line = ndp // 2
    cut = (cuts, cut_rows, width)
    (negative_sum,) = call(
        negative_kernel,
        2,
        ndp,
        nneg,
        (jax.ShapeDtypeStruct(cut, jnp.float32),),
        [pltpu.VMEM((line,) + cut, jnp.bfloat16)] * 5 + sems(*([line * cuts] * 6)),
        [vmem],
    )(negative_part.reshape((ndp,) + cut))
    negative_sum = negative_sum.reshape(negative_unit.shape)
    query_grad = (
        query_sum + positive_slope[:, None] * positive_unit.astype(jnp.float32)
    ) * inv_temp
    positive_grad = positive_slope[:, None] * query_unit.astype(jnp.float32) * inv_temp
    item_grad = jnp.concatenate([positive_grad, negative_sum * inv_temp], axis=0)
    query_grads = tower_backward(query_features, query_second, query_third, query_saved, query_grad)
    item_grads = tower_backward(item_features, item_second, item_third, item_saved, item_grad)
    gradients = query_grads + item_grads
    parts = [part for gradient in gradients for part in to_packed(gradient, ndp)]
    packed = jnp.concatenate(parts, axis=1)
    rows = packed.shape[1] // nneg
    packed = packed.reshape(ndp, nneg, 2, rows // 2, pack_columns).transpose(1, 0, 2, 3, 4)
    nx = nneg // 2
    piece = (rows // 2, pack_columns)
    bf16, f32 = jnp.bfloat16, jnp.float32
    gathered, stats = call(
        weight_kernel,
        3,
        ndp,
        nneg,
        (jax.ShapeDtypeStruct((nneg, 2) + piece, bf16), jax.ShapeDtypeStruct((8, 128), f32)),
        [
            pltpu.VMEM((nx, ndp, 2) + piece, bf16),
            pltpu.VMEM((nx, 2, line) + piece, bf16),
            pltpu.VMEM((2, nx, line) + piece, bf16),
            pltpu.VMEM((nx, 2, line) + piece, bf16),
            pltpu.VMEM((nx, line) + piece, bf16),
            pltpu.VMEM((2, line) + piece, bf16),
            pltpu.VMEM((nx, line) + piece, bf16),
            pltpu.VMEM((line,) + piece, bf16),
            pltpu.VMEM((nx, line) + piece, bf16),
            pltpu.VMEM((2, line) + piece, bf16),
            pltpu.VMEM((2, line) + piece, bf16),
            pltpu.VMEM((8, 128), f32),
            pltpu.VMEM((ndp, 8, 128), f32),
            pltpu.VMEM((8, 128), f32),
            pltpu.VMEM((nneg, 8, 128), f32),
        ]
        + sems(nx, nx, 2 * nx, 2 * nx, 2, 2, ndp, ndp, ndp, ndp, nneg, nneg, nx, nx, nx, nx),
        [vmem, pl.BlockSpec(memory_space=pltpu.SMEM)],
    )(packed, loss_part.reshape(1))
    grad_norm = jnp.sqrt(stats[0, 0])
    mean_loss = stats[0, 1] / (own_rows * ndp * nneg)
    clip_factor = clip_norm / jnp.maximum(grad_norm, clip_norm)
    flat = gathered.reshape(nneg * rows, pack_columns)
    clipped = []
    start = 0
    for gradient in gradients:
        height, columns = gradient.shape[0] // ndp, gradient.shape[1]
        groups = columns // pack_columns
        blocks = [flat[start + g * height : start + (g + 1) * height] for g in range(groups)]
        start += groups * height
        clipped.append(jnp.concatenate(blocks, axis=1).astype(jnp.float32) * clip_factor)
    return (mean_loss, *clipped)


def solution(mesh):
    placed = (
        P(("dp", "neg"), None),
        P(("dp", "neg"), None),
        P(("neg", "dp"), None),
        P("dp"),
        P(("dp", "neg")),
        P("neg"),
        P("neg"),
        P(),
        P(),
        P(),
        P(),
        P(),
        P(),
    )
    return jax.shard_map(
        per_device,
        mesh=mesh,
        in_specs=placed,
        out_specs=(
            P(),
            P("dp", None),
            P("dp", None),
            P("dp", None),
            P("dp", None),
            P("dp", None),
            P("dp", None),
        ),
        check_vma=False,
    )
```
